256 devices in a mesh: expert: 64 (over y, z_hi, x, core), group: 4 (over z_lo).
Axes of the slice: x: 4, y: 4, z: 8 (z_hi: 2, z_lo: 4; z = z_hi * 4 + z_lo), core: 2. Of those that a mesh axis runs over, the one named last changes fastest.
Arguments:
- tokens: bfloat16 [30720, 4096], P('expert', 'group'), may hold values from -6 to 6
- cotangent: bfloat16 [30720, 1024], P('expert'), may hold values from -6 to 6
- routing: int32 [30720, 1], P('expert'), may hold values from 0 to 63; in each aligned block of 480 rows (0 to 479, 480 to 959, ...) at most 15 rows name the same one
- stat_prev: float32 [64, 1024, 1024], P('expert', 'group'), as said below
- root_prev: bfloat16 [64, 1024, 1024], P('expert', 'group'), may hold values from -0.1875 to 0.1875
- owner_map: int32 [64], replicated, may hold values from 0 to 16, as said below
Outputs:
- statistic: float32 [64, 1024, 1024], P('expert', 'group')
- roots: bfloat16 [64, 1024, 1024], P('expert', 'group')
- update: bfloat16 [64, 4096, 1024], P('expert', 'group')
The draws below stay inside these ranges and needn't reach their ends.
Inputs may be any that keep to these rules, and one draw needn't show every extreme that they name: `routing`: in the rows of one device (aligned blocks of 480 rows) no expert is named more than 15 times, a bound that some block reaches. `owner_map`: A value below 16 names the index of expert that owns this expert's statistic; the value 16 marks a statistic that is not refreshed. Exactly 16 experts are refreshed; no owner holds more than 4 of them, and some owner holds exactly 4. `stat_prev`: each expert's block is symmetric and positive definite.
All inputs are finite; a program needn't handle non-finite values.
Results may differ from the reference program's by a relative error of at most 0.0055.
Values may be sent and summed in bfloat16 or wider, within the bound.
No kernel may reach another device: no remote copies, remote signals or barrier semaphores. Data moves between devices by JAX's collectives and lax.ppermute only.
A program may use at most 64 MiB of HBM per device.

```python
import math
import jax
import jax.numpy as jnp
import numpy as np
from jax import lax

D = 4096
FF = 1024
TOK_DEV = 480
ITERS = 2
POWER = 8
EXPERTS = 64
CAP = 15
OWNERS = 16
MOST = 4
REFRESH = 16
TOKENS = 30720
N_EXPERT = 64


def draw_stat_prev(key, part):
    diag_key = jax.random.fold_in(key, 11)
    mix_key = jax.random.fold_in(key, 12)
    low_end, high_end = (math.log(0.3), math.log(3.0))
    diagonal = jnp.exp(jax.random.uniform(diag_key, (EXPERTS, FF), jnp.float32, low_end, high_end))
    mixing = jax.random.normal(mix_key, (EXPERTS, FF, FF), jnp.float32)
    gram = jnp.einsum('eij,ekj->eik', mixing, mixing, precision=lax.Precision.HIGHEST) / (2.0 * FF)
    gram = 0.5 * (gram + jnp.swapaxes(gram, 1, 2))
    identity = (lax.broadcasted_iota(jnp.int32, (FF, FF), 0) == lax.broadcasted_iota(jnp.int32, (FF, FF), 1)).astype(jnp.float32)
    return gram + diagonal[:, :, None] * identity[None, :, :]


def draw_owner_map(key, part):
    order_key = jax.random.fold_in(key, 21)
    star_key = jax.random.fold_in(key, 22)
    other_key = jax.random.fold_in(key, 23)
    others_count = max(OWNERS - 1, 1)
    order = jax.random.permutation(order_key, EXPERTS)
    star = jax.random.randint(star_key, (), 0, OWNERS)
    others = (star + 1 + jax.random.permutation(other_key, others_count)) % OWNERS
    ranks = jnp.arange(REFRESH, dtype=jnp.int32)
    picked = jnp.where(ranks < MOST, star, others[jnp.maximum(ranks - MOST, 0) % others_count])
    result = jnp.full((EXPERTS,), OWNERS, jnp.int32)
    return result.at[order[:REFRESH]].set(picked.astype(jnp.int32))


def block_scale(stream_key, extent, split, smallest, high):
    def one(dim, shards_of):
        heights = jax.random.uniform(jax.random.fold_in(jax.random.fold_in(stream_key, 6), dim), (shards_of,), jnp.float32, smallest / len(split), high / len(split))
        return jnp.repeat(jnp.exp(heights), extent[dim] // shards_of).reshape((-1,) + (1,) * (len(extent) - dim - 1))

    factor_of = one(*split[0])
    for cut in split[1:]:
        factor_of = factor_of * one(*cut)
    return factor_of


def deal_out(own_key, own, number, rows, count, top, limit, lean):
    order = jax.random.permutation(own_key, count)
    crowded, ordinary = portions_of(count, rows * top, limit, lean, True), portions_of(count, rows * top, limit, lean, False)
    places = jnp.arange(count)

    def named(lengths, offset_by):
        used = int((lengths > 0).sum())
        fixed = max(1, used // 4)
        shifted = fixed + (places - fixed + offset_by * (used - fixed)) % max(1, count - fixed)
        return jnp.zeros((count,), jnp.int32).at[order[jnp.where(places < fixed, places, shifted)]].set(jnp.asarray(lengths, jnp.int32))

    lengths = jnp.where(number % 4 == 0, named(crowded, number // 4), named(ordinary, number - number // 4 - 1))
    mixed = jax.random.permutation(jax.random.fold_in(own, 3), count)
    source_of, taker = mixed[0:count // 2 * 2:2], mixed[1:count // 2 * 2:2]
    slack = jnp.minimum(lengths[source_of] - 1, limit - lengths[taker]) // 2
    slack = jnp.where((source_of == order[0]) | (taker == order[0]) | (lengths[taker] == 0), 0, jnp.maximum(slack, 0))
    shifted = jax.random.randint(jax.random.fold_in(own, 4), (count // 2,), 0, 1 << 20) % (slack + 1)
    lengths = lengths.at[source_of].add(-shifted).at[taker].add(shifted)
    labels = jnp.searchsorted(jnp.cumsum(lengths), jnp.arange(rows * top), side="right").astype(jnp.int32)
    grid = labels.reshape(top, rows).T
    grid = grid[jax.random.permutation(jax.random.fold_in(own, 1), rows)]
    offset_by = jax.random.randint(jax.random.fold_in(own, 2), (rows, 1), 0, top)
    return jnp.take_along_axis(grid, (jnp.arange(top)[None, :] + offset_by) % top, axis=1)


def portions_of(number_of, total, bound, skew, full):
    portions = [(1 << 20) // math.isqrt(rank ** skew) + 1 for rank in range(1, number_of + 1)]
    largest = bound if full else min(bound, max(-(-total // number_of), total * portions[0] // sum(portions)))
    least = 1 if total - largest >= number_of - 1 else 0
    holding, surplus = [largest] + [least] * (number_of - 1), total - largest - least * (number_of - 1)
    while surplus > 0:
        candidates = [i for i in range(1, number_of) if holding[i] < largest] or [i for i in range(1, number_of) if holding[i] < bound]
        whole, remaining = sum([portions[i] for i in candidates]), surplus
        for i in candidates:
            more = min(bound - holding[i], max(1, remaining * portions[i] // whole), surplus)
            holding[i] = holding[i] + more
            surplus = surplus - more
    return np.array(holding)


def centred(own_key, shape, width, reach, pieces=(), kind=jnp.bfloat16):
    level = block_scale(own_key, shape, pieces, -0.22, 0.18) if pieces else 1.0
    values = jax.random.normal(own_key, shape, jnp.float32) * width * level
    return jnp.minimum(jnp.maximum(values, -reach), reach).astype(kind)


def setup_inputs(seed: int = 0) -> dict:
    keys = jax.random.split(jax.random.key(seed), 7)
    tokens = centred(keys[0], (TOKENS, D), 1.0, 6.0, ((0, 64), (1, 4)))
    cotangent = centred(keys[1], (TOKENS, FF), 1.0, 6.0, ((0, 64),))
    routing_keys = jax.random.split(jax.random.fold_in(keys[2], 1), TOKENS // TOK_DEV)
    routing_turns = jax.random.permutation(jax.random.fold_in(keys[2], 3), TOKENS // TOK_DEV)
    routing = jax.vmap(lambda own, number: deal_out(jax.random.fold_in(keys[2], 2), own, number, TOK_DEV, EXPERTS, 1, CAP, 2))(routing_keys, routing_turns).reshape((TOKENS, 1))
    stat_prev = draw_stat_prev(jax.random.fold_in(keys[6], 71), 0)
    root_prev = centred(keys[4], (EXPERTS, FF, FF), FF ** -0.5, 0.1875, ((0, 64), (1, 4)))
    owner_map = draw_owner_map(jax.random.fold_in(keys[6], 71), 0)
    return {"tokens": tokens, "cotangent": cotangent, "routing": routing, "stat_prev": stat_prev, "root_prev": root_prev, "owner_map": owner_map}


keep_share = 0.9

def newton_root(block):
    order = block.shape[0]
    vector = jnp.full((order,), 1.0 / math.sqrt(order), jnp.float32)
    length = jnp.ones((), jnp.float32)
    for turn_index in range(POWER):
        image = jnp.dot(block, vector.astype(jnp.bfloat16), preferred_element_type=jnp.float32)
        length = jnp.sqrt(jnp.sum(image * image))
        vector = image / length
    scaling = 2.5 / length
    identity = (lax.broadcasted_iota(jnp.int32, (order, order), 0) == lax.broadcasted_iota(jnp.int32, (order, order), 1)).astype(jnp.float32)
    moment = scaling * block.astype(jnp.float32)
    moment_low = moment.astype(jnp.bfloat16)
    iterate = identity
    for turn_index in range(ITERS):
        factor = ((5.0 * identity - moment) * 0.25).astype(jnp.bfloat16)
        if turn_index == 0:
            iterate = factor.astype(jnp.float32)
        else:
            iterate = jnp.dot(iterate.astype(jnp.bfloat16), factor, preferred_element_type=jnp.float32)
        if turn_index + 1 < ITERS:
            square = jnp.dot(factor, factor, preferred_element_type=jnp.float32).astype(jnp.bfloat16)
            fourth = jnp.dot(square, square, preferred_element_type=jnp.float32).astype(jnp.bfloat16)
            moment = jnp.dot(fourth, moment_low, preferred_element_type=jnp.float32)
            moment_low = moment.astype(jnp.bfloat16)
    return (jnp.sqrt(jnp.sqrt(scaling)) * iterate).astype(jnp.bfloat16)

def reference(tokens, cotangent, routing, stat_prev, root_prev, owner_map):
    total_rows = tokens.shape[0]
    route = routing[:, 0]
    expert_ids = jnp.arange(EXPERTS, dtype=jnp.int32)
    onehot = (route[:, None] == expert_ids[None, :]).astype(jnp.int32)
    running = jnp.cumsum(onehot.reshape(N_EXPERT, TOK_DEV, EXPERTS), axis=1).reshape(total_rows, EXPERTS)
    position = lax.optimization_barrier(jnp.sum(onehot * (running - 1), axis=1)).astype(jnp.int32)
    source = jnp.arange(total_rows, dtype=jnp.int32) // TOK_DEV
    column = (source * CAP + position).astype(jnp.int32)
    table = jnp.full((EXPERTS, N_EXPERT * CAP), total_rows, jnp.int32)
    table = table.at[route, column].set(jnp.arange(total_rows, dtype=jnp.int32))
    tokens_pad = jnp.concatenate([tokens, jnp.zeros((1, tokens.shape[1]), tokens.dtype)], 0)
    signal_pad = jnp.concatenate([cotangent, jnp.zeros((1, cotangent.shape[1]), cotangent.dtype)], 0)
    grad_scale = 1.0 / math.sqrt(TOK_DEV)

    def per_expert(inputs):
        rows, previous, prior_root, owner = inputs
        taken = tokens_pad[rows]
        signal = signal_pad[rows]
        grad = lax.dot_general(taken, signal, (((0,), (0,)), ((), ())), preferred_element_type=jnp.float32)
        grad = (grad * grad_scale).astype(jnp.bfloat16)
        gram = lax.dot_general(grad, grad, (((0,), (0,)), ((), ())), preferred_element_type=jnp.float32)
        statistic = keep_share * previous + (1.0 - keep_share) * gram / D
        root = lax.cond(owner < OWNERS, lambda: newton_root(statistic.astype(jnp.bfloat16)), lambda: prior_root)
        update = jnp.dot(grad, root, preferred_element_type=jnp.float32).astype(jnp.bfloat16)
        return (statistic, root, update)
    stats, roots, updates = lax.map(per_expert, (table, stat_prev, root_prev, owner_map))
    return (stats, roots, updates)
```

```python
import functools
import math

import jax
import jax.numpy as jnp
from jax import lax
from jax.experimental import pallas as pl
from jax.experimental.pallas import tpu as pltpu
from jax.sharding import PartitionSpec as P

POWER = 8
KEEP = 0.9
SLOTS = 16
B = 128
PIECE = 9
MIB = 1024 * 1024


def vmem():
    return pl.BlockSpec(memory_space=pltpu.VMEM)


def smem():
    return pl.BlockSpec(memory_space=pltpu.SMEM)


def params(mib):
    return pltpu.CompilerParams(vmem_limit_bytes=mib * MIB)


def cost(flops, nbytes):
    return pl.CostEstimate(flops=int(flops), bytes_accessed=int(nbytes), transcendentals=0)


def outer(a, b):
    return lax.dot_general(a, b, (((0,), (0,)), ((), ())), preferred_element_type=jnp.float32)


def dot(a, b):
    return jnp.dot(a, b, preferred_element_type=jnp.float32)


def ones_where(mask):
    return jnp.where(mask, 1.0, 0.0).astype(jnp.bfloat16)


def dispatch_kernel(experts, rows, route_ref, tok_ref, sig_ref, out_ref, slot_ref):
    tokens = route_ref.shape[1]
    wide = tok_ref.shape[1]

    @pl.when(pl.program_id(0) == 0)
    def _():
        route = route_ref[...]
        hot = lax.broadcasted_iota(jnp.int32, (experts, tokens), 0) == route
        before = lax.broadcasted_iota(jnp.int32, (tokens, tokens), 0) < lax.broadcasted_iota(
            jnp.int32, (tokens, tokens), 1
        )
        earlier = dot(ones_where(hot), ones_where(before))
        position = jnp.sum(jnp.where(hot, earlier, 0.0), axis=0, keepdims=True)
        slot_ref[...] = route * SLOTS + position.astype(jnp.int32)

    at = lax.broadcasted_iota(jnp.int32, (rows, tokens), 0) + pl.program_id(0) * rows
    pick = ones_where(at == slot_ref[...])
    out_ref[:, :wide] = dot(pick, tok_ref[...]).astype(jnp.bfloat16)
    out_ref[:, wide:] = dot(pick, sig_ref[...]).astype(jnp.bfloat16)


def dispatch(route, tokens, signal, experts):
    count, wide = tokens.shape
    hidden = signal.shape[1]
    total, rows = experts * SLOTS, 256
    return pl.pallas_call(
        functools.partial(dispatch_kernel, experts, rows),
        grid=(total // rows,),
        in_specs=[
            pl.BlockSpec((1, count), lambda i: (0, 0)),
            pl.BlockSpec((count, wide), lambda i: (0, 0)),
            pl.BlockSpec((count, hidden), lambda i: (0, 0)),
        ],
        out_specs=pl.BlockSpec((rows, wide + hidden), lambda i: (i, 0)),
        out_shape=jax.ShapeDtypeStruct((total, wide + hidden), jnp.bfloat16),
        scratch_shapes=[pltpu.VMEM((1, count), jnp.int32)],
        compiler_params=params(24),
        cost_estimate=cost(2 * total * count * (wide + hidden), 6 * MIB),
        name="dispatch",
    )(route, tokens, signal)


def owned_blocks(d, group):
    found = [(d, d, 0, 0), (d, d, 0, 1), (d, d, 1, 1)]
    for h in range(group):
        if h > d:
            found += [(d, h, 0, 0), (d, h, 0, 1)]
        if h < d:
            found += [(h, d, 1, 0), (h, d, 1, 1)]
    return found


def gradient_kernel(group, scale, x_ref, grad_ref, part_ref):
    wide = grad_ref.shape[0]
    step = 2 * B
    for r in range(wide // step):
        block = outer(x_ref[:, r * step : (r + 1) * step], x_ref[:, wide:])
        grad_ref[r * step : (r + 1) * step, :] = (block * scale).astype(jnp.bfloat16)
    place = {}
    for d in range(group):
        for k, name in enumerate(owned_blocks(d, group)):
            place[name] = (d, k)
    for p in range(group):
        for q in range(p, group):
            gram = outer(
                grad_ref[:, p * step : (p + 1) * step], grad_ref[:, q * step : (q + 1) * step]
            ).astype(jnp.bfloat16)
            for i in range(2):
                for j in range(2):
                    if (p, q, i, j) in place:
                        d, k = place[(p, q, i, j)]
                        part_ref[d, k * B : (k + 1) * B, :] = gram[
                            i * B : (i + 1) * B, j * B : (j + 1) * B
                        ]


def gradient(x, group, wide, scale):
    total, both = x.shape
    hidden = both - wide
    return pl.pallas_call(
        functools.partial(gradient_kernel, group, scale),
        in_specs=[vmem()],
        out_specs=(vmem(), vmem()),
        out_shape=(
            jax.ShapeDtypeStruct((wide, hidden), jnp.bfloat16),
            jax.ShapeDtypeStruct((group, PIECE * B, B), jnp.bfloat16),
        ),
        compiler_params=params(32),
        cost_estimate=cost(2 * wide * hidden * (total + hidden), 8 * MIB),
        name="gradient",
    )(x)


def statistic_kernel(group, full, me_ref, parts_ref, prev_ref, stat_ref, own_ref):
    me = me_ref[0]

    def gram(k):
        total = parts_ref[0, k * B : (k + 1) * B, :].astype(jnp.float32)
        for s in range(1, group):
            total += parts_ref[s, k * B : (k + 1) * B, :].astype(jnp.float32)
        return total

    def put(k, block, row, col):
        at = (slice(row, row + B), pl.ds(pl.multiple_of(col, B), B))
        new = KEEP * prev_ref[at] + (1.0 - KEEP) * block / full
        stat_ref[at] = new
        own_ref[k * B : (k + 1) * B, :] = new.astype(jnp.bfloat16)

    mine = me * 2 * B
    put(0, gram(0), 0, mine)
    put(1, gram(1), 0, mine + B)
    put(2, gram(2), B, mine + B)
    for j in range(group - 1):
        k = 3 + 2 * j

        @pl.when(j >= me)
        def _():
            col = (j + 1) * 2 * B
            put(k, gram(k), 0, col)
            put(k + 1, gram(k + 1), 0, col + B)

        @pl.when(j < me)
        def _():
            col = j * 2 * B + B
            put(k, gram(k).T, 0, col)
            put(k + 1, gram(k + 1).T, B, col)


def new_statistic(me, parts, prev, full):
    group = parts.shape[0]
    return pl.pallas_call(
        functools.partial(statistic_kernel, group, float(full)),
        in_specs=[smem(), vmem(), vmem()],
        out_specs=(vmem(), vmem()),
        out_shape=(
            jax.ShapeDtypeStruct(prev.shape, jnp.float32),
            jax.ShapeDtypeStruct((PIECE * B, B), jnp.bfloat16),
        ),
        compiler_params=params(16),
        cost_estimate=cost(4 * prev.size, 4 * MIB),
        name="statistic",
    )(me, parts, prev)


def root_kernel(group, flags_ref, pieces_ref, part_ref, stat_ref, root_ref, a_ref, f_ref, g_ref, h_ref):
    me, live = flags_ref[0], flags_ref[1]
    order = a_ref.shape[0]
    step = 2 * B

    def fill(block, row, col, mirror=True):
        a_ref[row : row + B, col : col + B] = block
        if mirror:
            a_ref[col : col + B, row : row + B] = block.T

    for s in range(group):
        at = s * step
        block = [pieces_ref[s, k * B : (k + 1) * B, :] for k in range(PIECE)]
        fill(block[0], at, at, False)
        fill(block[1], at, at + B)
        fill(block[2], at + B, at + B, False)
        k = 3
        for h in range(group):
            if h > s:
                fill(block[k], at, h * step)
                fill(block[k + 1], at, h * step + B)
            if h < s:
                fill(block[k], at, h * step + B)
                fill(block[k + 1], at + B, h * step + B)
            if h != s:
                k += 2

    row = lax.broadcasted_iota(jnp.int32, (step, step), 0)
    col = lax.broadcasted_iota(jnp.int32, (step, step), 1)
    mine = pl.multiple_of(me * step, step)
    for h in range(group):
        own = (row < jnp.where(h < me, 0, B)) | (col >= jnp.where(h > me, step, B))
        low = a_ref[pl.ds(mine, step), h * step : (h + 1) * step].astype(jnp.float32)
        at = (slice(None), slice(h * step, (h + 1) * step))
        stat_ref[at] = jnp.where(own, part_ref[at], low)

    @pl.when(live != 0)
    def _():
        def power(_, carry):
            vector, _ = carry
            image = dot(vector.astype(jnp.bfloat16), a_ref[...])
            length = jnp.sqrt(jnp.sum(image * image, axis=1, keepdims=True))
            return image / length, length

        vector = jnp.full((16, order), 1.0 / math.sqrt(order), jnp.float32)
        length = jnp.ones((16, 1), jnp.float32)
        _, length = lax.fori_loop(0, POWER, power, (vector, length))
        scaling = 2.5 / length[:1, :1]
        quarter = jnp.sqrt(jnp.sqrt(scaling)) * 0.25

        def rows_of(i):
            return pl.ds(pl.multiple_of(i * step, step), step)

        def first(i, _):
            here = rows_of(i)
            line = lax.broadcasted_iota(jnp.int32, (step, order), 0) + i * step
            eye = line == lax.broadcasted_iota(jnp.int32, (step, order), 1)
            moment = scaling * a_ref[here, :].astype(jnp.float32)
            f_ref[here, :] = ((jnp.where(eye, 5.0, 0.0) - moment) * 0.25).astype(jnp.bfloat16)
            return 0

        lax.fori_loop(0, order // step, first, 0)

        def second(i, _):
            here = rows_of(i)
            factor = f_ref[here, :]
            square = dot(factor, f_ref[...])
            g_ref[here, :] = square.astype(jnp.bfloat16)
            h_ref[here, :] = (5.0 * factor.astype(jnp.float32) - 4.0 * square).astype(jnp.bfloat16)
            return 0

        lax.fori_loop(0, order // step, second, 0)

        def third(i, _):
            here = rows_of(i)
            a_ref[here, :] = dot(g_ref[here, :], g_ref[...]).astype(jnp.bfloat16)
            return 0

        lax.fori_loop(0, order // step, third, 0)

        def last(i, _):
            here = rows_of(i)
            tail = dot(a_ref[here, :], h_ref[...])
            factor = f_ref[here, :].astype(jnp.float32)
            root_ref[here, :] = ((5.0 * factor - tail) * quarter).astype(jnp.bfloat16)
            return 0

        lax.fori_loop(0, order // step, last, 0)


def inverse_root(flags, pieces, part, order):
    group = pieces.shape[0]
    square = pltpu.VMEM((order, order), jnp.bfloat16)
    return pl.pallas_call(
        functools.partial(root_kernel, group),
        in_specs=[smem(), vmem(), vmem()],
        out_specs=(vmem(), vmem()),
        out_shape=(
            jax.ShapeDtypeStruct(part.shape, jnp.float32),
            jax.ShapeDtypeStruct((order, order), jnp.bfloat16),
        ),
        scratch_shapes=[square] * 4,
        compiler_params=params(32),
        cost_estimate=cost(6 * order**3, 8 * MIB),
        name="root",
    )(flags, pieces, part)


def update_kernel(group, flags_ref, grad_ref, root_ref, *refs):
    prev_refs, (update_ref, rows_ref, whole_ref) = refs[:group], refs[group:]
    me, live = flags_ref[0], flags_ref[1]
    step = prev_refs[0].shape[0]

    def rows_of(i):
        return pl.ds(pl.multiple_of(i * step, step), step)

    @pl.when(live != 0)
    def _():
        rows_ref[...] = root_ref[rows_of(me), :]

        def line(i, _):
            here = rows_of(i)
            update_ref[here, :] = dot(grad_ref[here, :], root_ref[...]).astype(jnp.bfloat16)
            return 0

        lax.fori_loop(0, grad_ref.shape[0] // step, line, 0)

    @pl.when(live == 0)
    def _():
        rows_ref[...] = prev_refs[0][...]
        for k in range(group):
            source = lax.rem(me - k + group, group)
            whole_ref[rows_of(source), :] = prev_refs[k][...]

        def line(i, _):
            here = rows_of(i)
            update_ref[here, :] = dot(grad_ref[here, :], whole_ref[...]).astype(jnp.bfloat16)
            return 0

        lax.fori_loop(0, grad_ref.shape[0] // step, line, 0)


def updated(flags, grad, root, prevs):
    group = len(prevs)
    wide, order = grad.shape
    return pl.pallas_call(
        functools.partial(update_kernel, group),
        in_specs=[smem()] + [vmem()] * (2 + group),
        out_specs=(vmem(), vmem()),
        out_shape=(
            jax.ShapeDtypeStruct((wide, order), jnp.bfloat16),
            jax.ShapeDtypeStruct(prevs[0].shape, jnp.bfloat16),
        ),
        scratch_shapes=[pltpu.VMEM((order, order), jnp.bfloat16)],
        compiler_params=params(32),
        cost_estimate=cost(2 * wide * order * order, 8 * MIB),
        name="update",
    )(flags, grad, root, *prevs)


def body(tokens, cotangent, routing, stat_prev, root_prev, owner_map):
    experts = lax.axis_size("expert")
    group = lax.axis_size("group")
    my_expert = lax.axis_index("expert")
    me = lax.axis_index("group").astype(jnp.int32)
    rows, wide = tokens.shape
    order = cotangent.shape[1]
    owners = experts // 4
    live = (jnp.take(owner_map, my_expert) < owners).astype(jnp.int32)
    flags = jnp.stack([me, live])

    sent = dispatch(routing.reshape(1, rows), tokens, cotangent, experts)
    sent = sent.reshape(experts, SLOTS, wide + order)
    got = lax.all_to_all(sent, "expert", 0, 0, tiled=True)
    got = got.reshape(experts * SLOTS, wide + order)
    grad, part = gradient(got, group, wide, 1.0 / math.sqrt(rows))
    parts = lax.all_to_all(part, "group", 0, 0, tiled=True)
    stat_own, own = new_statistic(flags, parts, stat_prev[0], wide * group)
    copies = jnp.broadcast_to(own[None], (group,) + own.shape)
    pieces = lax.all_to_all(copies, "group", 0, 0, tiled=True)
    prev, pieces = lax.optimization_barrier((root_prev[0], pieces))
    prevs = [prev]
    for k in range(1, group):
        ring = [(g, (g + k) % group) for g in range(group)]
        prevs.append(lax.ppermute(prev, "group", ring))
    stat, root = inverse_root(flags, pieces, stat_own, order)
    update, root_rows = updated(flags, grad, root, prevs)
    return stat[None], root_rows[None], update[None]


def solution(mesh):
    in_specs = (
        P("expert", "group"),
        P("expert", None),
        P("expert", None),
        P("expert", "group", None),
        P("expert", "group", None),
        P(),
    )
    out_specs = (P("expert", "group", None), P("expert", "group", None), P("expert", "group", None))
    return jax.shard_map(body, mesh=mesh, in_specs=in_specs, out_specs=out_specs, check_vma=False)
```

```python
import functools
import math

import jax
import jax.numpy as jnp
from jax import lax
from jax.experimental import pallas as pl
from jax.experimental.pallas import tpu as pltpu
from jax.sharding import PartitionSpec as P

POWER = 8
KEEP = 0.9
SLOTS = 16
B = 128
HALF = 8
PIECE = 9
MIB = 1024 * 1024


def vmem():
    return pl.BlockSpec(memory_space=pltpu.VMEM)


def smem():
    return pl.BlockSpec(memory_space=pltpu.SMEM)


def params(mib):
    return pltpu.CompilerParams(vmem_limit_bytes=mib * MIB)


def cost(flops, nbytes):
    return pl.CostEstimate(flops=int(flops), bytes_accessed=int(nbytes), transcendentals=0)


def outer(a, b):
    return lax.dot_general(a, b, (((0,), (0,)), ((), ())), preferred_element_type=jnp.float32)


def dot(a, b):
    return jnp.dot(a, b, preferred_element_type=jnp.float32)


def ones_where(mask):
    return jnp.where(mask, 1.0, 0.0).astype(jnp.bfloat16)


def dispatch_kernel(experts, route_hbm, tok_hbm, sig_hbm, out_ref, route_ref, slot_ref, tok_ref, sig_ref, sems):
    tokens = route_ref.shape[1]
    wide = tok_ref.shape[1]
    rows = out_ref.shape[0]

    @pl.when(pl.program_id(0) == 0)
    def _():
        copies = [
            pltpu.make_async_copy(route_hbm, route_ref, sems.at[0]),
            pltpu.make_async_copy(tok_hbm, tok_ref, sems.at[1]),
            pltpu.make_async_copy(sig_hbm, sig_ref, sems.at[2]),
        ]
        for copy in copies:
            copy.start()
        before = lax.broadcasted_iota(jnp.int32, (tokens, tokens), 0) < lax.broadcasted_iota(
            jnp.int32, (tokens, tokens), 1
        )
        before = ones_where(before)
        copies[0].wait()
        route = route_ref[...]
        hot = lax.broadcasted_iota(jnp.int32, (experts, tokens), 0) == route
        earlier = dot(ones_where(hot), before)
        position = jnp.sum(jnp.where(hot, earlier, 0.0), axis=0, keepdims=True)
        slot_ref[...] = route * SLOTS + position.astype(jnp.int32)
        copies[1].wait()
        copies[2].wait()

    at = lax.broadcasted_iota(jnp.int32, (rows, tokens), 0) + pl.program_id(0) * rows
    pick = ones_where(at == slot_ref[...])
    out_ref[:, :wide] = dot(pick, tok_ref[...]).astype(jnp.bfloat16)
    out_ref[:, wide:] = dot(pick, sig_ref[...]).astype(jnp.bfloat16)


def dispatch(route, tokens, signal, experts):
    count, wide = tokens.shape
    hidden = signal.shape[1]
    total, rows = experts * SLOTS, 2 * B
    return pl.pallas_call(
        functools.partial(dispatch_kernel, experts),
        grid=(total // rows,),
        in_specs=[pl.BlockSpec(memory_space=pl.ANY)] * 3,
        out_specs=pl.BlockSpec((rows, wide + hidden), lambda i: (i, 0)),
        out_shape=jax.ShapeDtypeStruct((total, wide + hidden), jnp.bfloat16),
        scratch_shapes=[
            pltpu.VMEM((1, count), jnp.int32),
            pltpu.VMEM((1, count), jnp.int32),
            pltpu.VMEM((count, wide), jnp.bfloat16),
            pltpu.VMEM((count, hidden), jnp.bfloat16),
            pltpu.SemaphoreType.DMA((3,)),
        ],
        compiler_params=params(60),
        cost_estimate=cost(2 * total * count * (wide + hidden), 6 * MIB),
        name="dispatch",
    )(route, tokens, signal)


def owned_blocks(d, group):
    found = [(d, d, 0, 0), (d, d, 0, 1), (d, d, 1, 1)]
    for h in range(group):
        if h > d:
            found += [(d, h, 0, 0), (d, h, 0, 1)]
        if h < d:
            found += [(h, d, 1, 0), (h, d, 1, 1)]
    return found


def gradient_kernel(group, scale, x_hbm, grad_hbm, part_hbm, x_ref, grad_ref, part_ref, sems):
    wide = grad_ref.shape[0]
    step = 2 * B
    lines = wide // step
    loads = [pltpu.make_async_copy(x_hbm.at[:, wide:], x_ref.at[:, wide:], sems.at[0])]
    stores = []
    for r in range(lines):
        at = slice(r * step, (r + 1) * step)
        loads.append(pltpu.make_async_copy(x_hbm.at[:, at], x_ref.at[:, at], sems.at[1 + r]))
        stores.append(pltpu.make_async_copy(grad_ref.at[at, :], grad_hbm.at[at, :], sems.at[1 + lines + r]))
    for load in loads:
        load.start()
    loads[0].wait()
    for r in range(lines):
        loads[1 + r].wait()
        at = slice(r * step, (r + 1) * step)
        grad_ref[at, :] = (outer(x_ref[:, at], x_ref[:, wide:]) * scale).astype(jnp.bfloat16)
        stores[r].start()
    place = {}
    for d in range(group):
        for k, name in enumerate(owned_blocks(d, group)):
            place[name] = (d, k)
    last = {d: max((p, q) for (p, q, _, _) in owned_blocks(d, group)) for d in range(group)}
    for p in range(group):
        for q in range(p, group):
            gram = outer(
                grad_ref[:, p * step : (p + 1) * step], grad_ref[:, q * step : (q + 1) * step]
            ).astype(jnp.bfloat16)
            for i in range(2):
                for j in range(2):
                    if (p, q, i, j) in place:
                        d, k = place[(p, q, i, j)]
                        part_ref[d, k * B : (k + 1) * B, :] = gram[
                            i * B : (i + 1) * B, j * B : (j + 1) * B
                        ]
            for d in range(group):
                if last[d] == (p, q):
                    sem = sems.at[1 + 2 * lines + d]
                    stores.append(pltpu.make_async_copy(part_ref.at[d], part_hbm.at[d], sem))
                    stores[-1].start()
    for store in stores:
        store.wait()


def gradient(x, group, wide, scale):
    total, both = x.shape
    hidden = both - wide
    part = (group, PIECE * B, B)
    return pl.pallas_call(
        functools.partial(gradient_kernel, group, scale),
        in_specs=[pl.BlockSpec(memory_space=pl.ANY)],
        out_specs=(pl.BlockSpec(memory_space=pl.ANY),) * 2,
        out_shape=(
            jax.ShapeDtypeStruct((wide, hidden), jnp.bfloat16),
            jax.ShapeDtypeStruct(part, jnp.bfloat16),
        ),
        scratch_shapes=[
            pltpu.VMEM(x.shape, jnp.bfloat16),
            pltpu.VMEM((wide, hidden), jnp.bfloat16),
            pltpu.VMEM(part, jnp.bfloat16),
            pltpu.SemaphoreType.DMA((1 + 2 * (wide // (2 * B)) + group,)),
        ],
        compiler_params=params(60),
        cost_estimate=cost(2 * wide * hidden * (total + hidden), 10 * MIB),
        name="gradient",
    )(x)


def statistic_kernel(
    group, full, flags_ref, parts_ref, prev_ref, root_ref, stat_hbm, send_ref, stat_ref, own_ref, sem
):
    me, live = flags_ref[0], flags_ref[1]

    def gram(k):
        total = parts_ref[0, k * B : (k + 1) * B, :].astype(jnp.float32)
        for s in range(1, group):
            total += parts_ref[s, k * B : (k + 1) * B, :].astype(jnp.float32)
        return total

    def put(k, block, row, col):
        at = (slice(row, row + B), pl.ds(pl.multiple_of(col, B), B))
        new = KEEP * prev_ref[at] + (1.0 - KEEP) * block / full
        stat_ref[at] = new
        own_ref[k * B : (k + 1) * B, :] = new.astype(jnp.bfloat16)

    mine = pl.multiple_of(me * 2 * B, 2 * B)
    put(0, gram(0), 0, mine)
    put(1, gram(1), 0, mine + B)
    put(2, gram(2), B, mine + B)
    for j in range(group - 1):
        k = 3 + 2 * j

        @pl.when(j >= me)
        def _():
            col = (j + 1) * 2 * B
            put(k, gram(k), 0, col)
            put(k + 1, gram(k + 1), 0, col + B)

        @pl.when(j < me)
        def _():
            col = j * 2 * B + B
            put(k, gram(k).T, 0, col)
            put(k + 1, gram(k + 1).T, B, col)

    stat_ref[B:, pl.ds(mine, B)] = stat_ref[:B, pl.ds(mine + B, B)].T
    store = pltpu.make_async_copy(stat_ref, stat_hbm, sem)
    store.start()

    @pl.when(live != 0)
    def _():
        for t in range(group):
            send_ref[t, : PIECE * B, :] = own_ref[...]

    @pl.when(live == 0)
    def _():
        for t in range(group):
            for c in range(HALF):
                send_ref[t, (2 + c) * B : (3 + c) * B, :] = root_ref[B:, c * B : (c + 1) * B]
            send_ref[t, : 2 * B, :] = own_ref[pl.ds(shared(me, t), 2 * B), :]

    store.wait()


def shared(s, t):
    other = jnp.where(t > s, t - 1, jnp.minimum(t, PIECE // 2 - 2))
    return pl.multiple_of((3 + 2 * other) * B, B)


def new_statistic(flags, parts, prev, root, full):
    group = parts.shape[0]
    return pl.pallas_call(
        functools.partial(statistic_kernel, group, float(full)),
        in_specs=[smem(), vmem(), vmem(), vmem()],
        out_specs=(pl.BlockSpec(memory_space=pl.ANY), vmem()),
        out_shape=(
            jax.ShapeDtypeStruct(prev.shape, jnp.float32),
            jax.ShapeDtypeStruct((group, (2 + HALF) * B, B), jnp.bfloat16),
        ),
        scratch_shapes=[
            pltpu.VMEM(prev.shape, jnp.float32),
            pltpu.VMEM((PIECE * B, B), jnp.bfloat16),
            pltpu.SemaphoreType.DMA,
        ],
        compiler_params=params(8),
        cost_estimate=cost(4 * prev.size, 4 * MIB),
        name="statistic",
    )(flags, parts, prev, root)


def root_kernel(
    group,
    flags_ref,
    pieces_ref,
    prev_ref,
    grad_hbm,
    part_hbm,
    stat_hbm,
    rows_ref,
    update_hbm,
    a_ref,
    f_ref,
    g_ref,
    h_ref,
    grad_ref,
    mirror_ref,
    sems,
):
    me, live = flags_ref[0], flags_ref[1]
    order = a_ref.shape[0]
    step = 2 * B
    done = sems.at[2 * group - 2]
    load = pltpu.make_async_copy(grad_hbm, grad_ref, sems.at[2 * group - 1])

    @pl.when(live != 0)
    def _():
        load.start()

    def mirrored(j):
        s = jnp.where(j < me, j, j + 1)
        start = jnp.where(live != 0, shared(s, me), 0)
        col = pl.multiple_of(s * step, step)
        found = []
        for k in range(2):
            at = pl.ds(pl.multiple_of(start + k * B, B), B)
            mirror_ref[2 * j + k] = pieces_ref[s, at, :].astype(jnp.float32).T
            row = jnp.where(j < me, k * B, B)
            place = col + jnp.where(j < me, 0, k * B)
            target = stat_hbm.at[pl.ds(pl.multiple_of(row, B), B), pl.ds(pl.multiple_of(place, B), B)]
            found.append(pltpu.make_async_copy(mirror_ref.at[2 * j + k], target, sems.at[2 * j + k]))
        return found

    stores = []
    for j in range(group - 1):
        stores += mirrored(j)
        stores[-2].start()
        stores[-1].start()
    @pl.when(live == 0)
    def _():
        rows_ref[...] = prev_ref[...]
        for s in range(group):
            for c in range(HALF):
                a_ref[s * B : (s + 1) * B, c * B : (c + 1) * B] = pieces_ref[
                    s, (2 + c) * B : (3 + c) * B, :
                ]
        held = slice(0, group * B)
        store = pltpu.make_async_copy(a_ref.at[held, :], update_hbm.at[held, :], done)
        store.start()
        store.wait()

    @pl.when(live != 0)
    def _():
        def fill(block, row, col, mirror=True):
            a_ref[row : row + B, col : col + B] = block
            if mirror:
                a_ref[col : col + B, row : row + B] = block.T

        for s in range(group):
            at = s * step
            block = [pieces_ref[s, k * B : (k + 1) * B, :] for k in range(PIECE)]
            fill(block[0], at, at, False)
            fill(block[1], at, at + B)
            fill(block[2], at + B, at + B, False)
            k = 3
            for h in range(group):
                if h > s:
                    fill(block[k], at, h * step)
                    fill(block[k + 1], at, h * step + B)
                if h < s:
                    fill(block[k], at, h * step + B)
                    fill(block[k + 1], at + B, h * step + B)
                if h != s:
                    k += 2

        def power(_, carry):
            vector, _ = carry
            image = dot(vector.astype(jnp.bfloat16), a_ref[...])
            length = jnp.sqrt(jnp.sum(image * image, axis=1, keepdims=True))
            return image / length, length

        vector = jnp.full((16, order), 1.0 / math.sqrt(order), jnp.float32)
        length = jnp.ones((16, 1), jnp.float32)
        _, length = lax.fori_loop(0, POWER, power, (vector, length))
        scaling = 2.5 / length[:1, :1]
        quarter = jnp.sqrt(jnp.sqrt(scaling)) * 0.25

        def rows_of(i):
            return pl.ds(pl.multiple_of(i * step, step), step)

        def first(i, _):
            here = rows_of(i)
            line = lax.broadcasted_iota(jnp.int32, (step, order), 0) + i * step
            eye = line == lax.broadcasted_iota(jnp.int32, (step, order), 1)
            moment = scaling * a_ref[here, :].astype(jnp.float32)
            f_ref[here, :] = ((jnp.where(eye, 5.0, 0.0) - moment) * 0.25).astype(jnp.bfloat16)
            return 0

        lax.fori_loop(0, order // step, first, 0)

        def second(i, _):
            here = rows_of(i)
            factor = f_ref[here, :]
            square = dot(factor, f_ref[...])
            g_ref[here, :] = square.astype(jnp.bfloat16)
            h_ref[here, :] = (5.0 * factor.astype(jnp.float32) - 4.0 * square).astype(jnp.bfloat16)
            return 0

        lax.fori_loop(0, order // step, second, 0)

        def third(i, _):
            here = rows_of(i)
            a_ref[here, :] = dot(g_ref[here, :], g_ref[...]).astype(jnp.bfloat16)
            return 0

        lax.fori_loop(0, order // step, third, 0)

        def last(i, _):
            here = rows_of(i)
            tail = dot(a_ref[here, :], h_ref[...])
            factor = f_ref[here, :].astype(jnp.float32)
            g_ref[here, :] = ((5.0 * factor - tail) * quarter).astype(jnp.bfloat16)
            return 0

        lax.fori_loop(0, order // step, last, 0)
        rows_ref[...] = g_ref[rows_of(me), :]
        load.wait()

        def line(i, _):
            here = rows_of(i)
            f_ref[here, :] = dot(grad_ref[here, :], g_ref[...]).astype(jnp.bfloat16)
            pltpu.make_async_copy(f_ref.at[here, :], update_hbm.at[here, :], done).start()
            return 0

        lax.fori_loop(0, order // step, line, 0)
        pltpu.make_async_copy(f_ref, update_hbm, done).wait()

    for store in stores:
        store.wait()


def inverse_root(flags, pieces, prev, grad, part):
    group = pieces.shape[0]
    wide, order = grad.shape
    square = pltpu.VMEM((order, order), jnp.bfloat16)
    anywhere = pl.BlockSpec(memory_space=pl.ANY)
    return pl.pallas_call(
        functools.partial(root_kernel, group),
        in_specs=[smem(), vmem(), vmem(), anywhere, anywhere],
        out_specs=(anywhere, vmem(), anywhere),
        out_shape=(
            jax.ShapeDtypeStruct(part.shape, jnp.float32),
            jax.ShapeDtypeStruct(prev.shape, jnp.bfloat16),
            jax.ShapeDtypeStruct(grad.shape, jnp.bfloat16),
        ),
        input_output_aliases={4: 0},
        scratch_shapes=[square] * 4
        + [
            pltpu.VMEM(grad.shape, jnp.bfloat16),
            pltpu.VMEM((2 * (group - 1), B, B), jnp.float32),
            pltpu.SemaphoreType.DMA((2 * group,)),
        ],
        compiler_params=params(60),
        cost_estimate=cost(10 * order**3, 8 * MIB),
        name="root",
    )(flags, pieces, prev, grad, part)


def kept_kernel(
    group, flags_ref, late_hbm, grad_hbm, old_hbm, update_hbm, late_ref, grad_ref, half_ref, whole_ref, new_ref, sems
):
    live = flags_ref[1]
    step = 2 * B

    @pl.when(live == 0)
    def _():
        loads = [
            pltpu.make_async_copy(late_hbm, late_ref, sems.at[2]),
            pltpu.make_async_copy(old_hbm.at[: group * B, :], half_ref, sems.at[0]),
            pltpu.make_async_copy(grad_hbm, grad_ref, sems.at[3]),
        ]
        for load in loads:
            load.start()
        loads[0].wait()
        for s in range(group):
            whole_ref[s * step : s * step + B, :] = late_ref[s]
        loads[1].wait()
        for s in range(group):
            whole_ref[s * step + B : (s + 1) * step, :] = half_ref[s * B : (s + 1) * B, :]
        loads[2].wait()

        def line(i, _):
            here = pl.ds(pl.multiple_of(i * step, step), step)
            new_ref[here, :] = dot(grad_ref[here, :], whole_ref[...]).astype(jnp.bfloat16)
            pltpu.make_async_copy(new_ref.at[here, :], update_hbm.at[here, :], sems.at[1]).start()
            return 0

        lax.fori_loop(0, grad_ref.shape[0] // step, line, 0)
        pltpu.make_async_copy(new_ref, update_hbm, sems.at[1]).wait()


def kept_update(flags, late, grad, update):
    group = late.shape[0]
    wide, order = grad.shape
    anywhere = pl.BlockSpec(memory_space=pl.ANY)
    square = pltpu.VMEM((order, order), jnp.bfloat16)
    return pl.pallas_call(
        functools.partial(kept_kernel, group),
        in_specs=[smem(), anywhere, anywhere, anywhere],
        out_specs=anywhere,
        out_shape=jax.ShapeDtypeStruct(grad.shape, jnp.bfloat16),
        input_output_aliases={3: 0},
        scratch_shapes=[
            pltpu.VMEM(late.shape, jnp.bfloat16),
            pltpu.VMEM(grad.shape, jnp.bfloat16),
            pltpu.VMEM((group * B, order), jnp.bfloat16),
            square,
            pltpu.VMEM(grad.shape, jnp.bfloat16),
            pltpu.SemaphoreType.DMA((4,)),
        ],
        compiler_params=params(60),
        cost_estimate=cost(2 * wide * order * order, 8 * MIB),
        name="kept",
    )(flags, late, grad, update)


def body(tokens, cotangent, routing, stat_prev, root_prev, owner_map):
    experts = lax.axis_size("expert")
    group = lax.axis_size("group")
    my_expert = lax.axis_index("expert")
    me = lax.axis_index("group").astype(jnp.int32)
    rows, wide = tokens.shape
    order = cotangent.shape[1]
    owners = experts // 4
    live = (jnp.take(owner_map, my_expert) < owners).astype(jnp.int32)
    flags = jnp.stack([me, live])

    prev = root_prev[0]
    sent = dispatch(routing.reshape(1, rows), tokens, cotangent, experts)
    sent = sent.reshape(experts, SLOTS, wide + order)
    got = lax.all_to_all(sent, "expert", 0, 0, tiled=True)
    grad, part = gradient(got.reshape(experts * SLOTS, -1), group, wide, 1.0 / math.sqrt(rows))
    part, later = lax.optimization_barrier((part, prev))
    parts = lax.all_to_all(part, "group", 0, 0, tiled=True)
    late = jnp.broadcast_to(later[:B][None], (group, B, order))
    parts, late = lax.optimization_barrier((parts, late))
    stat_own, send = new_statistic(flags, parts, stat_prev[0], prev, wide * group)
    pieces = lax.all_to_all(send, "group", 0, 0, tiled=True)
    pieces, late = lax.optimization_barrier((pieces, late))
    late = lax.all_to_all(late, "group", 0, 0, tiled=True)
    stat, root_rows, update = inverse_root(flags, pieces, prev, grad, stat_own)
    update = kept_update(flags, late, grad, update)
    return stat[None], root_rows[None], update[None]


def solution(mesh):
    in_specs = (
        P("expert", "group"),
        P("expert", None),
        P("expert", None),
        P("expert", "group", None),
        P("expert", "group", None),
        P(),
    )
    out_specs = (P("expert", "group", None), P("expert", "group", None), P("expert", "group", None))
    return jax.shard_map(body, mesh=mesh, in_specs=in_specs, out_specs=out_specs, check_vma=False)
```

```python
import functools
import math

import jax
import jax.numpy as jnp
from jax import lax
from jax.experimental import pallas as pl
from jax.experimental.pallas import tpu as pltpu
from jax.sharding import PartitionSpec as P


POWER = 8
KEEP = 0.9
SLOTS = 16
B = 128
HALF = 8
PIECE = 9
MIB = 1024 * 1024


def vmem():
    return pl.BlockSpec(memory_space=pltpu.VMEM)


def smem():
    return pl.BlockSpec(memory_space=pltpu.SMEM)


def params(mib):
    return pltpu.CompilerParams(vmem_limit_bytes=mib * MIB)


def cost(flops, nbytes):
    return pl.CostEstimate(flops=int(flops), bytes_accessed=int(nbytes), transcendentals=0)


def outer(a, b):
    return lax.dot_general(a, b, (((0,), (0,)), ((), ())), preferred_element_type=jnp.float32)


def dot(a, b):
    return jnp.dot(a, b, preferred_element_type=jnp.float32)


def ones_where(mask):
    return jnp.where(mask, 1.0, 0.0).astype(jnp.bfloat16)


def dispatch_kernel(experts, route_hbm, tok_hbm, sig_hbm, out_ref, route_ref, slot_ref, tok_ref, sig_ref, sems):
    tokens = route_ref.shape[1]
    wide = tok_ref.shape[1]
    rows = out_ref.shape[0]

    @pl.when(pl.program_id(0) == 0)
    def _():
        copies = [
            pltpu.make_async_copy(route_hbm, route_ref, sems.at[0]),
            pltpu.make_async_copy(tok_hbm, tok_ref, sems.at[1]),
            pltpu.make_async_copy(sig_hbm, sig_ref, sems.at[2]),
        ]
        for copy in copies:
            copy.start()
        before = lax.broadcasted_iota(jnp.int32, (tokens, tokens), 0) < lax.broadcasted_iota(
            jnp.int32, (tokens, tokens), 1
        )
        before = ones_where(before)
        copies[0].wait()
        route = route_ref[...]
        hot = lax.broadcasted_iota(jnp.int32, (experts, tokens), 0) == route
        earlier = dot(ones_where(hot), before)
        position = jnp.sum(jnp.where(hot, earlier, 0.0), axis=0, keepdims=True)
        slot_ref[...] = route * SLOTS + position.astype(jnp.int32)
        copies[1].wait()
        copies[2].wait()

    at = lax.broadcasted_iota(jnp.int32, (rows, tokens), 0) + pl.program_id(0) * rows
    pick = ones_where(at == slot_ref[...])
    out_ref[:, :wide] = dot(pick, tok_ref[...]).astype(jnp.bfloat16)
    out_ref[:, wide:] = dot(pick, sig_ref[...]).astype(jnp.bfloat16)


def dispatch(route, tokens, signal, experts):
    count, wide = tokens.shape
    hidden = signal.shape[1]
    total, rows = experts * SLOTS, 2 * B
    return pl.pallas_call(
        functools.partial(dispatch_kernel, experts),
        grid=(total // rows,),
        in_specs=[pl.BlockSpec(memory_space=pl.ANY)] * 3,
        out_specs=pl.BlockSpec((rows, wide + hidden), lambda i: (i, 0)),
        out_shape=jax.ShapeDtypeStruct((total, wide + hidden), jnp.bfloat16),
        scratch_shapes=[
            pltpu.VMEM((1, count), jnp.int32),
            pltpu.VMEM((1, count), jnp.int32),
            pltpu.VMEM((count, wide), jnp.bfloat16),
            pltpu.VMEM((count, hidden), jnp.bfloat16),
            pltpu.SemaphoreType.DMA((3,)),
        ],
        compiler_params=params(60),
        cost_estimate=cost(2 * total * count * (wide + hidden), 6 * MIB),
        name="dispatch",
    )(route, tokens, signal)


def owned_blocks(d, group):
    found = [(d, d, 0, 0), (d, d, 0, 1), (d, d, 1, 1)]
    for h in range(group):
        if h > d:
            found += [(d, h, 0, 0), (d, h, 0, 1)]
        if h < d:
            found += [(h, d, 1, 0), (h, d, 1, 1)]
    return found


def gradient_kernel(group, scale, x_hbm, grad_hbm, part_hbm, x_ref, grad_ref, part_ref, sems):
    wide = grad_ref.shape[0]
    step = 2 * B
    lines = wide // step
    loads = [pltpu.make_async_copy(x_hbm.at[:, wide:], x_ref.at[:, wide:], sems.at[0])]
    stores = []
    for r in range(lines):
        at = slice(r * step, (r + 1) * step)
        loads.append(pltpu.make_async_copy(x_hbm.at[:, at], x_ref.at[:, at], sems.at[1 + r]))
        stores.append(pltpu.make_async_copy(grad_ref.at[at, :], grad_hbm.at[at, :], sems.at[1 + lines + r]))
    for load in loads:
        load.start()
    loads[0].wait()
    for r in range(lines):
        loads[1 + r].wait()
        at = slice(r * step, (r + 1) * step)
        grad_ref[at, :] = (outer(x_ref[:, at], x_ref[:, wide:]) * scale).astype(jnp.bfloat16)
        stores[r].start()
    place = {}
    for d in range(group):
        for k, name in enumerate(owned_blocks(d, group)):
            place[name] = (d, k)
    last = {d: max((p, q) for (p, q, _, _) in owned_blocks(d, group)) for d in range(group)}
    for p in range(group):
        for q in range(p, group):
            gram = outer(
                grad_ref[:, p * step : (p + 1) * step], grad_ref[:, q * step : (q + 1) * step]
            ).astype(jnp.bfloat16)
            for i in range(2):
                for j in range(2):
                    if (p, q, i, j) in place:
                        d, k = place[(p, q, i, j)]
                        part_ref[d, k * B : (k + 1) * B, :] = gram[
                            i * B : (i + 1) * B, j * B : (j + 1) * B
                        ]
            for d in range(group):
                if last[d] == (p, q):
                    sem = sems.at[1 + 2 * lines + d]
                    stores.append(pltpu.make_async_copy(part_ref.at[d], part_hbm.at[d], sem))
                    stores[-1].start()
    for store in stores:
        store.wait()


def gradient(x, group, wide, scale):
    total, both = x.shape
    hidden = both - wide
    part = (group, PIECE * B, B)
    return pl.pallas_call(
        functools.partial(gradient_kernel, group, scale),
        in_specs=[pl.BlockSpec(memory_space=pl.ANY)],
        out_specs=(pl.BlockSpec(memory_space=pl.ANY),) * 2,
        out_shape=(
            jax.ShapeDtypeStruct((wide, hidden), jnp.bfloat16),
            jax.ShapeDtypeStruct(part, jnp.bfloat16),
        ),
        scratch_shapes=[
            pltpu.VMEM(x.shape, jnp.bfloat16),
            pltpu.VMEM((wide, hidden), jnp.bfloat16),
            pltpu.VMEM(part, jnp.bfloat16),
            pltpu.SemaphoreType.DMA((1 + 2 * (wide // (2 * B)) + group,)),
        ],
        compiler_params=params(60),
        cost_estimate=cost(2 * wide * hidden * (total + hidden), 10 * MIB),
        name="gradient",
    )(x)


def statistic_kernel(
    group, full, flags_ref, parts_ref, prev_ref, root_ref, stat_hbm, send_ref, stat_ref, own_ref, sem
):
    me, live = flags_ref[0], flags_ref[1]

    def gram(k):
        total = parts_ref[0, k * B : (k + 1) * B, :].astype(jnp.float32)
        for s in range(1, group):
            total += parts_ref[s, k * B : (k + 1) * B, :].astype(jnp.float32)
        return total

    def put(k, block, row, col):
        at = (slice(row, row + B), pl.ds(pl.multiple_of(col, B), B))
        new = KEEP * prev_ref[at] + (1.0 - KEEP) * block / full
        stat_ref[at] = new
        own_ref[k * B : (k + 1) * B, :] = new.astype(jnp.bfloat16)

    mine = pl.multiple_of(me * 2 * B, 2 * B)
    put(0, gram(0), 0, mine)
    put(1, gram(1), 0, mine + B)
    put(2, gram(2), B, mine + B)
    for j in range(group - 1):
        k = 3 + 2 * j

        @pl.when(j >= me)
        def _():
            col = (j + 1) * 2 * B
            put(k, gram(k), 0, col)
            put(k + 1, gram(k + 1), 0, col + B)

        @pl.when(j < me)
        def _():
            col = j * 2 * B + B
            put(k, gram(k).T, 0, col)
            put(k + 1, gram(k + 1).T, B, col)

    stat_ref[B:, pl.ds(mine, B)] = stat_ref[:B, pl.ds(mine + B, B)].T
    store = pltpu.make_async_copy(stat_ref, stat_hbm, sem)
    store.start()

    @pl.when(live != 0)
    def _():
        for t in range(group):
            send_ref[t, : PIECE * B, :] = own_ref[...]

    @pl.when(live == 0)
    def _():
        for t in range(group):
            for c in range(HALF):
                send_ref[t, (2 + c) * B : (3 + c) * B, :] = root_ref[B:, c * B : (c + 1) * B]
            send_ref[t, : 2 * B, :] = own_ref[pl.ds(shared(me, t), 2 * B), :]

    store.wait()


def shared(s, t):
    other = jnp.where(t > s, t - 1, jnp.minimum(t, PIECE // 2 - 2))
    return pl.multiple_of((3 + 2 * other) * B, B)


def new_statistic(flags, parts, prev, root, full):
    group = parts.shape[0]
    return pl.pallas_call(
        functools.partial(statistic_kernel, group, float(full)),
        in_specs=[smem(), vmem(), vmem(), vmem()],
        out_specs=(pl.BlockSpec(memory_space=pl.ANY), vmem()),
        out_shape=(
            jax.ShapeDtypeStruct(prev.shape, jnp.float32),
            jax.ShapeDtypeStruct((group, (2 + HALF) * B, B), jnp.bfloat16),
        ),
        scratch_shapes=[
            pltpu.VMEM(prev.shape, jnp.float32),
            pltpu.VMEM((PIECE * B, B), jnp.bfloat16),
            pltpu.SemaphoreType.DMA,
        ],
        compiler_params=params(8),
        cost_estimate=cost(4 * prev.size, 4 * MIB),
        name="statistic",
    )(flags, parts, prev, root)


def root_kernel(
    group,
    flags_ref,
    pieces_ref,
    prev_ref,
    grad_hbm,
    part_hbm,
    stat_hbm,
    rows_ref,
    update_hbm,
    a_ref,
    f_ref,
    g_ref,
    h_ref,
    grad_ref,
    mirror_ref,
    sems,
):
    me, live = flags_ref[0], flags_ref[1]
    order = a_ref.shape[0]
    step = 2 * B
    done = sems.at[2 * group - 2]
    load = pltpu.make_async_copy(grad_hbm, grad_ref, sems.at[2 * group - 1])

    @pl.when(live != 0)
    def _():
        load.start()

    def mirrored(j):
        s = jnp.where(j < me, j, j + 1)
        start = jnp.where(live != 0, shared(s, me), 0)
        col = pl.multiple_of(s * step, step)
        found = []
        for k in range(2):
            at = pl.ds(pl.multiple_of(start + k * B, B), B)
            mirror_ref[2 * j + k] = pieces_ref[s, at, :].astype(jnp.float32).T
            row = jnp.where(j < me, k * B, B)
            place = col + jnp.where(j < me, 0, k * B)
            target = stat_hbm.at[pl.ds(pl.multiple_of(row, B), B), pl.ds(pl.multiple_of(place, B), B)]
            found.append(pltpu.make_async_copy(mirror_ref.at[2 * j + k], target, sems.at[2 * j + k]))
        return found

    stores = []
    for j in range(group - 1):
        stores += mirrored(j)
        stores[-2].start()
        stores[-1].start()

    @pl.when(live == 0)
    def _():
        rows_ref[...] = prev_ref[...]
        for s in range(group):
            for c in range(HALF):
                a_ref[s * B : (s + 1) * B, c * B : (c + 1) * B] = pieces_ref[
                    s, (2 + c) * B : (3 + c) * B, :
                ]
        held = slice(0, group * B)
        store = pltpu.make_async_copy(a_ref.at[held, :], update_hbm.at[held, :], done)
        store.start()
        store.wait()

    @pl.when(live != 0)
    def _():
        def fill(block, row, col, mirror=True):
            a_ref[row : row + B, col : col + B] = block
            if mirror:
                a_ref[col : col + B, row : row + B] = block.T

        for s in range(group):
            at = s * step
            block = [pieces_ref[s, k * B : (k + 1) * B, :] for k in range(PIECE)]
            fill(block[0], at, at, False)
            fill(block[1], at, at + B)
            fill(block[2], at + B, at + B, False)
            k = 3
            for h in range(group):
                if h > s:
                    fill(block[k], at, h * step)
                    fill(block[k + 1], at, h * step + B)
                if h < s:
                    fill(block[k], at, h * step + B)
                    fill(block[k + 1], at + B, h * step + B)
                if h != s:
                    k += 2

        def power(_, carry):
            vector, _ = carry
            image = dot(vector.astype(jnp.bfloat16), a_ref[...])
            length = jnp.sqrt(jnp.sum(image * image, axis=1, keepdims=True))
            return image / length, length

        vector = jnp.full((16, order), 1.0 / math.sqrt(order), jnp.float32)
        length = jnp.ones((16, 1), jnp.float32)
        _, length = lax.fori_loop(0, POWER, power, (vector, length))
        scaling = 2.5 / length[:1, :1]
        quarter = jnp.sqrt(jnp.sqrt(scaling)) * 0.25

        def rows_of(i):
            return pl.ds(pl.multiple_of(i * step, step), step)

        def first(i, _):
            here = rows_of(i)
            line = lax.broadcasted_iota(jnp.int32, (step, order), 0) + i * step
            eye = line == lax.broadcasted_iota(jnp.int32, (step, order), 1)
            moment = scaling * a_ref[here, :].astype(jnp.float32)
            f_ref[here, :] = ((jnp.where(eye, 5.0, 0.0) - moment) * 0.25).astype(jnp.bfloat16)
            return 0

        lax.fori_loop(0, order // step, first, 0)

        def second(i, _):
            here = rows_of(i)
            factor = f_ref[here, :]
            square = dot(factor, f_ref[...])
            g_ref[here, :] = square.astype(jnp.bfloat16)
            h_ref[here, :] = (5.0 * factor.astype(jnp.float32) - 4.0 * square).astype(jnp.bfloat16)
            return 0

        lax.fori_loop(0, order // step, second, 0)

        def third(i, _):
            here = rows_of(i)
            a_ref[here, :] = dot(g_ref[here, :], g_ref[...]).astype(jnp.bfloat16)
            return 0

        lax.fori_loop(0, order // step, third, 0)

        def last(i, _):
            here = rows_of(i)
            tail = dot(a_ref[here, :], h_ref[...])
            factor = f_ref[here, :].astype(jnp.float32)
            g_ref[here, :] = ((5.0 * factor - tail) * quarter).astype(jnp.bfloat16)
            return 0

        lax.fori_loop(0, order // step, last, 0)
        rows_ref[...] = g_ref[rows_of(me), :]
        load.wait()

        def line(i, _):
            here = rows_of(i)
            f_ref[here, :] = dot(grad_ref[here, :], g_ref[...]).astype(jnp.bfloat16)
            pltpu.make_async_copy(f_ref.at[here, :], update_hbm.at[here, :], done).start()
            return 0

        lax.fori_loop(0, order // step, line, 0)
        pltpu.make_async_copy(f_ref, update_hbm, done).wait()

    for store in stores:
        store.wait()


def inverse_root(flags, pieces, prev, grad, part):
    group = pieces.shape[0]
    _, order = grad.shape
    square = pltpu.VMEM((order, order), jnp.bfloat16)
    anywhere = pl.BlockSpec(memory_space=pl.ANY)
    return pl.pallas_call(
        functools.partial(root_kernel, group),
        in_specs=[smem(), vmem(), vmem(), anywhere, anywhere],
        out_specs=(anywhere, vmem(), anywhere),
        out_shape=(
            jax.ShapeDtypeStruct(part.shape, jnp.float32),
            jax.ShapeDtypeStruct(prev.shape, jnp.bfloat16),
            jax.ShapeDtypeStruct(grad.shape, jnp.bfloat16),
        ),
        input_output_aliases={4: 0},
        scratch_shapes=[square] * 4
        + [
            pltpu.VMEM(grad.shape, jnp.bfloat16),
            pltpu.VMEM((2 * (group - 1), B, B), jnp.float32),
            pltpu.SemaphoreType.DMA((2 * group,)),
        ],
        compiler_params=params(60),
        cost_estimate=cost(10 * order**3, 8 * MIB),
        name="root",
    )(flags, pieces, prev, grad, part)


def kept_kernel(
    group, flags_ref, first_hbm, prev_hbm, second_hbm, third_hbm, grad_hbm, old_hbm, update_hbm, *scratch
):
    upper_ref, grad_ref, half_ref, whole_ref, new_ref, sems = scratch
    me, live = flags_ref[0], flags_ref[1]
    step = 2 * B

    @pl.when(live == 0)
    def _():
        uppers = (prev_hbm.at[:B, :], first_hbm, second_hbm, third_hbm)
        loads = [pltpu.make_async_copy(uppers[k], upper_ref.at[k], sems.at[k]) for k in range(group)]
        loads.append(pltpu.make_async_copy(old_hbm.at[: group * B, :], half_ref, sems.at[group]))
        loads.append(pltpu.make_async_copy(grad_hbm, grad_ref, sems.at[group + 1]))
        for load in loads:
            load.start()
        for k in range(group):
            loads[k].wait()
            source = lax.rem(me - k + group, group)
            whole_ref[pl.ds(pl.multiple_of(source * step, step), B), :] = upper_ref[k]
        loads[group].wait()
        for s in range(group):
            whole_ref[s * step + B : (s + 1) * step, :] = half_ref[s * B : (s + 1) * B, :]
        loads[group + 1].wait()

        def line(i, _):
            here = pl.ds(pl.multiple_of(i * step, step), step)
            new_ref[here, :] = dot(grad_ref[here, :], whole_ref[...]).astype(jnp.bfloat16)
            pltpu.make_async_copy(new_ref.at[here, :], update_hbm.at[here, :], sems.at[group + 2]).start()
            return 0

        lax.fori_loop(0, grad_ref.shape[0] // step, line, 0)
        pltpu.make_async_copy(new_ref, update_hbm, sems.at[group + 2]).wait()


def kept_update(flags, first, prev, second, third, grad, update):
    group = 4
    wide, order = grad.shape
    anywhere = pl.BlockSpec(memory_space=pl.ANY)
    return pl.pallas_call(
        functools.partial(kept_kernel, group),
        in_specs=[smem()] + [anywhere] * 6,
        out_specs=anywhere,
        out_shape=jax.ShapeDtypeStruct(grad.shape, jnp.bfloat16),
        input_output_aliases={6: 0},
        scratch_shapes=[
            pltpu.VMEM((group, B, order), jnp.bfloat16),
            pltpu.VMEM(grad.shape, jnp.bfloat16),
            pltpu.VMEM((group * B, order), jnp.bfloat16),
            pltpu.VMEM((order, order), jnp.bfloat16),
            pltpu.VMEM(grad.shape, jnp.bfloat16),
            pltpu.SemaphoreType.DMA((group + 3,)),
        ],
        compiler_params=params(60),
        cost_estimate=cost(2 * wide * order * order, 8 * MIB),
        name="kept",
    )(flags, first, prev, second, third, grad, update)


def step_of(tokens, cotangent, routing, stat_prev, root_prev, owner_map):
    experts = lax.axis_size("expert")
    group = lax.axis_size("group")
    my_expert = lax.axis_index("expert")
    me = lax.axis_index("group").astype(jnp.int32)
    rows, wide = tokens.shape
    order = cotangent.shape[1]
    owners = experts // 4
    live = (jnp.take(owner_map, my_expert) < owners).astype(jnp.int32)
    flags = jnp.stack([me, live])

    def shifted(x, k):
        return lax.ppermute(x, "group", [(g, (g + k) % group) for g in range(group)])

    prev = root_prev[0]
    upper = prev[:B]
    from_1 = shifted(upper, 1)
    from_3 = shifted(upper, 3)
    sent = dispatch(routing.reshape(1, rows), tokens, cotangent, experts)
    sent = sent.reshape(experts, SLOTS, wide + order)
    got = lax.all_to_all(sent, "expert", 0, 0, tiled=True)
    grad, part = gradient(got.reshape(experts * SLOTS, -1), group, wide, 1.0 / math.sqrt(rows))
    parts = lax.all_to_all(part, "group", 0, 0, tiled=True)
    stat_own, send = new_statistic(flags, parts, stat_prev[0], prev, wide * group)
    pieces = lax.all_to_all(send, "group", 0, 0, tiled=True)
    pieces, upper = lax.optimization_barrier((pieces, upper))
    from_2 = shifted(upper, 2)
    stat, root_rows, update = inverse_root(flags, pieces, prev, grad, stat_own)
    update = kept_update(flags, from_1, prev, from_2, from_3, grad, update)
    return stat[None], root_rows[None], update[None]


def solution(mesh):
    in_specs = (
        P("expert", "group"),
        P("expert", None),
        P("expert", None),
        P("expert", "group", None),
        P("expert", "group", None),
        P(),
    )
    out_specs = (P("expert", "group", None), P("expert", "group", None), P("expert", "group", None))
    return jax.shard_map(step_of, mesh=mesh, in_specs=in_specs, out_specs=out_specs, check_vma=False)
```

```python
import functools
import math

import jax
import jax.numpy as jnp
from jax import lax
from jax.experimental import pallas as pl
from jax.experimental.pallas import tpu as pltpu
from jax.sharding import PartitionSpec as P


POWER = 8
KEEP = 0.9
SLOTS = 16
B = 128
HALF = 8
PIECE = 9
MIB = 1024 * 1024


def vmem():
    return pl.BlockSpec(memory_space=pltpu.VMEM)


def smem():
    return pl.BlockSpec(memory_space=pltpu.SMEM)


def params(mib):
    return pltpu.CompilerParams(vmem_limit_bytes=mib * MIB)


def cost(flops, nbytes):
    return pl.CostEstimate(flops=int(flops), bytes_accessed=int(nbytes), transcendentals=0)


def outer(a, b):
    return lax.dot_general(a, b, (((0,), (0,)), ((), ())), preferred_element_type=jnp.float32)


def dot(a, b):
    return jnp.dot(a, b, preferred_element_type=jnp.float32)


def ones_where(mask):
    return jnp.where(mask, 1.0, 0.0).astype(jnp.bfloat16)


def dispatch_kernel(experts, route_hbm, tok_hbm, sig_hbm, out_ref, route_ref, slot_ref, tok_ref, sig_ref, sems):
    tokens = route_ref.shape[1]
    wide = tok_ref.shape[1]
    rows = out_ref.shape[0]

    @pl.when(pl.program_id(0) == 0)
    def _():
        copies = [
            pltpu.make_async_copy(route_hbm, route_ref, sems.at[0]),
            pltpu.make_async_copy(tok_hbm, tok_ref, sems.at[1]),
            pltpu.make_async_copy(sig_hbm, sig_ref, sems.at[2]),
        ]
        for copy in copies:
            copy.start()
        before = lax.broadcasted_iota(jnp.int32, (tokens, tokens), 0) < lax.broadcasted_iota(
            jnp.int32, (tokens, tokens), 1
        )
        before = ones_where(before)
        copies[0].wait()
        route = route_ref[...]
        hot = lax.broadcasted_iota(jnp.int32, (experts, tokens), 0) == route
        earlier = dot(ones_where(hot), before)
        position = jnp.sum(jnp.where(hot, earlier, 0.0), axis=0, keepdims=True)
        slot_ref[...] = route * SLOTS + position.astype(jnp.int32)
        copies[1].wait()
        copies[2].wait()

    at = lax.broadcasted_iota(jnp.int32, (rows, tokens), 0) + pl.program_id(0) * rows
    pick = ones_where(at == slot_ref[...])
    out_ref[:, :wide] = dot(pick, tok_ref[...]).astype(jnp.bfloat16)
    out_ref[:, wide:] = dot(pick, sig_ref[...]).astype(jnp.bfloat16)


def dispatch(route, tokens, signal, experts):
    count, wide = tokens.shape
    hidden = signal.shape[1]
    total, rows = experts * SLOTS, 2 * B
    return pl.pallas_call(
        functools.partial(dispatch_kernel, experts),
        grid=(total // rows,),
        in_specs=[pl.BlockSpec(memory_space=pl.ANY)] * 3,
        out_specs=pl.BlockSpec((rows, wide + hidden), lambda i: (i, 0)),
        out_shape=jax.ShapeDtypeStruct((total, wide + hidden), jnp.bfloat16),
        scratch_shapes=[
            pltpu.VMEM((1, count), jnp.int32),
            pltpu.VMEM((1, count), jnp.int32),
            pltpu.VMEM((count, wide), jnp.bfloat16),
            pltpu.VMEM((count, hidden), jnp.bfloat16),
            pltpu.SemaphoreType.DMA((3,)),
        ],
        compiler_params=params(60),
        cost_estimate=cost(2 * total * count * (wide + hidden), 6 * MIB),
        name="dispatch",
    )(route, tokens, signal)


def owned_blocks(d, group):
    found = [(d, d, 0, 0), (d, d, 0, 1), (d, d, 1, 1)]
    for h in range(group):
        if h > d:
            found += [(d, h, 0, 0), (d, h, 0, 1)]
        if h < d:
            found += [(h, d, 1, 0), (h, d, 1, 1)]
    return found


def gradient_kernel(group, scale, x_hbm, grad_hbm, part_hbm, x_ref, grad_ref, part_ref, sems):
    wide = grad_ref.shape[0]
    step = 2 * B
    lines = wide // step
    loads = [pltpu.make_async_copy(x_hbm.at[:, wide:], x_ref.at[:, wide:], sems.at[0])]
    stores = []
    for r in range(lines):
        at = slice(r * step, (r + 1) * step)
        loads.append(pltpu.make_async_copy(x_hbm.at[:, at], x_ref.at[:, at], sems.at[1 + r]))
        stores.append(pltpu.make_async_copy(grad_ref.at[at, :], grad_hbm.at[at, :], sems.at[1 + lines + r]))
    for load in loads:
        load.start()
    loads[0].wait()
    for r in range(lines):
        loads[1 + r].wait()
        at = slice(r * step, (r + 1) * step)
        grad_ref[at, :] = (outer(x_ref[:, at], x_ref[:, wide:]) * scale).astype(jnp.bfloat16)
        stores[r].start()
    place = {}
    for d in range(group):
        for k, name in enumerate(owned_blocks(d, group)):
            place[name] = (d, k)
    last = {d: max((p, q) for (p, q, _, _) in owned_blocks(d, group)) for d in range(group)}
    for p in range(group):
        for q in range(p, group):
            gram = outer(
                grad_ref[:, p * step : (p + 1) * step], grad_ref[:, q * step : (q + 1) * step]
            ).astype(jnp.bfloat16)
            for i in range(2):
                for j in range(2):
                    if (p, q, i, j) in place:
                        d, k = place[(p, q, i, j)]
                        part_ref[d, k * B : (k + 1) * B, :] = gram[
                            i * B : (i + 1) * B, j * B : (j + 1) * B
                        ]
            for d in range(group):
                if last[d] == (p, q):
                    sem = sems.at[1 + 2 * lines + d]
                    stores.append(pltpu.make_async_copy(part_ref.at[d], part_hbm.at[d], sem))
                    stores[-1].start()
    for store in stores:
        store.wait()


def gradient(x, group, wide, scale):
    total, both = x.shape
    hidden = both - wide
    part = (group, PIECE * B, B)
    return pl.pallas_call(
        functools.partial(gradient_kernel, group, scale),
        in_specs=[pl.BlockSpec(memory_space=pl.ANY)],
        out_specs=(pl.BlockSpec(memory_space=pl.ANY),) * 2,
        out_shape=(
            jax.ShapeDtypeStruct((wide, hidden), jnp.bfloat16),
            jax.ShapeDtypeStruct(part, jnp.bfloat16),
        ),
        scratch_shapes=[
            pltpu.VMEM(x.shape, jnp.bfloat16),
            pltpu.VMEM((wide, hidden), jnp.bfloat16),
            pltpu.VMEM(part, jnp.bfloat16),
            pltpu.SemaphoreType.DMA((1 + 2 * (wide // (2 * B)) + group,)),
        ],
        compiler_params=params(60),
        cost_estimate=cost(2 * wide * hidden * (total + hidden), 10 * MIB),
        name="gradient",
    )(x)


def statistic_kernel(
    group, full, flags_ref, parts_ref, prev_ref, root_ref, stat_hbm, send_ref, stat_ref, own_ref, sem
):
    me, live = flags_ref[0], flags_ref[1]

    def gram(k):
        total = parts_ref[0, k * B : (k + 1) * B, :].astype(jnp.float32)
        for s in range(1, group):
            total += parts_ref[s, k * B : (k + 1) * B, :].astype(jnp.float32)
        return total

    def put(k, block, row, col):
        at = (slice(row, row + B), pl.ds(pl.multiple_of(col, B), B))
        new = KEEP * prev_ref[at] + (1.0 - KEEP) * block / full
        stat_ref[at] = new
        own_ref[k * B : (k + 1) * B, :] = new.astype(jnp.bfloat16)

    mine = pl.multiple_of(me * 2 * B, 2 * B)
    put(0, gram(0), 0, mine)
    put(1, gram(1), 0, mine + B)
    put(2, gram(2), B, mine + B)
    for j in range(group - 1):
        k = 3 + 2 * j

        @pl.when(j >= me)
        def _():
            col = (j + 1) * 2 * B
            put(k, gram(k), 0, col)
            put(k + 1, gram(k + 1), 0, col + B)

        @pl.when(j < me)
        def _():
            col = j * 2 * B + B
            put(k, gram(k).T, 0, col)
            put(k + 1, gram(k + 1).T, B, col)

    stat_ref[B:, pl.ds(mine, B)] = stat_ref[:B, pl.ds(mine + B, B)].T
    store = pltpu.make_async_copy(stat_ref, stat_hbm, sem)
    store.start()

    @pl.when(live != 0)
    def _():
        for t in range(group):
            send_ref[t, : PIECE * B, :] = own_ref[...]

    @pl.when(live == 0)
    def _():
        for t in range(group):
            for c in range(HALF):
                send_ref[t, (2 + c) * B : (3 + c) * B, :] = root_ref[B:, c * B : (c + 1) * B]
            send_ref[t, : 2 * B, :] = own_ref[pl.ds(shared(me, t), 2 * B), :]

    store.wait()


def shared(s, t):
    other = jnp.where(t > s, t - 1, jnp.minimum(t, PIECE // 2 - 2))
    return pl.multiple_of((3 + 2 * other) * B, B)


def new_statistic(flags, parts, prev, root, full):
    group = parts.shape[0]
    return pl.pallas_call(
        functools.partial(statistic_kernel, group, float(full)),
        in_specs=[smem(), vmem(), vmem(), vmem()],
        out_specs=(pl.BlockSpec(memory_space=pl.ANY), vmem()),
        out_shape=(
            jax.ShapeDtypeStruct(prev.shape, jnp.float32),
            jax.ShapeDtypeStruct((group, (2 + HALF) * B, B), jnp.bfloat16),
        ),
        scratch_shapes=[
            pltpu.VMEM(prev.shape, jnp.float32),
            pltpu.VMEM((PIECE * B, B), jnp.bfloat16),
            pltpu.SemaphoreType.DMA,
        ],
        compiler_params=params(8),
        cost_estimate=cost(4 * prev.size, 4 * MIB),
        name="statistic",
    )(flags, parts, prev, root)


def root_kernel(
    group,
    flags_ref,
    pieces_ref,
    prev_ref,
    first_hbm,
    second_hbm,
    third_hbm,
    grad_hbm,
    part_hbm,
    stat_hbm,
    rows_ref,
    update_hbm,
    a_ref,
    f_ref,
    g_ref,
    h_ref,
    grad_ref,
    upper_ref,
    mirror_ref,
    sems,
):
    me, live = flags_ref[0], flags_ref[1]
    order = a_ref.shape[0]
    step = 2 * B
    done = sems.at[2 * group - 2]
    load = pltpu.make_async_copy(grad_hbm, grad_ref, sems.at[2 * group - 1])
    uppers = [
        pltpu.make_async_copy(source, upper_ref.at[k], sems.at[2 * group + k])
        for k, source in enumerate((first_hbm, second_hbm, third_hbm))
    ]
    load.start()

    @pl.when(live == 0)
    def _():
        for upper in uppers:
            upper.start()

    def mirrored(j):
        s = jnp.where(j < me, j, j + 1)
        start = jnp.where(live != 0, shared(s, me), 0)
        col = pl.multiple_of(s * step, step)
        found = []
        for k in range(2):
            at = pl.ds(pl.multiple_of(start + k * B, B), B)
            mirror_ref[2 * j + k] = pieces_ref[s, at, :].astype(jnp.float32).T
            row = jnp.where(j < me, k * B, B)
            place = col + jnp.where(j < me, 0, k * B)
            target = stat_hbm.at[pl.ds(pl.multiple_of(row, B), B), pl.ds(pl.multiple_of(place, B), B)]
            found.append(pltpu.make_async_copy(mirror_ref.at[2 * j + k], target, sems.at[2 * j + k]))
        return found

    stores = []
    for j in range(group - 1):
        stores += mirrored(j)
        stores[-2].start()
        stores[-1].start()

    def rows_of(i, count=step):
        return pl.ds(pl.multiple_of(i * step, step), count)

    @pl.when(live == 0)
    def _():
        rows_ref[...] = prev_ref[...]
        for s in range(group):
            for c in range(HALF):
                g_ref[s * step + B : (s + 1) * step, c * B : (c + 1) * B] = pieces_ref[
                    s, (2 + c) * B : (3 + c) * B, :
                ]
        g_ref[rows_of(me, B), :] = prev_ref[:B, :]
        for k in range(1, group):
            uppers[k - 1].wait()
            g_ref[rows_of(lax.rem(me - k + group, group), B), :] = upper_ref[k - 1]

    @pl.when(live != 0)
    def _():
        def fill(block, row, col, mirror=True):
            a_ref[row : row + B, col : col + B] = block
            if mirror:
                a_ref[col : col + B, row : row + B] = block.T

        for s in range(group):
            at = s * step
            block = [pieces_ref[s, k * B : (k + 1) * B, :] for k in range(PIECE)]
            fill(block[0], at, at, False)
            fill(block[1], at, at + B)
            fill(block[2], at + B, at + B, False)
            k = 3
            for h in range(group):
                if h > s:
                    fill(block[k], at, h * step)
                    fill(block[k + 1], at, h * step + B)
                if h < s:
                    fill(block[k], at, h * step + B)
                    fill(block[k + 1], at + B, h * step + B)
                if h != s:
                    k += 2

        def power(_, carry):
            vector, _ = carry
            image = dot(vector.astype(jnp.bfloat16), a_ref[...])
            length = jnp.sqrt(jnp.sum(image * image, axis=1, keepdims=True))
            return image / length, length

        vector = jnp.full((16, order), 1.0 / math.sqrt(order), jnp.float32)
        length = jnp.ones((16, 1), jnp.float32)
        _, length = lax.fori_loop(0, POWER, power, (vector, length))
        scaling = 2.5 / length[:1, :1]
        quarter = jnp.sqrt(jnp.sqrt(scaling)) * 0.25

        def first(i, _):
            here = rows_of(i)
            line = lax.broadcasted_iota(jnp.int32, (step, order), 0) + i * step
            eye = line == lax.broadcasted_iota(jnp.int32, (step, order), 1)
            moment = scaling * a_ref[here, :].astype(jnp.float32)
            f_ref[here, :] = ((jnp.where(eye, 5.0, 0.0) - moment) * 0.25).astype(jnp.bfloat16)
            return 0

        lax.fori_loop(0, order // step, first, 0)

        def second(i, _):
            here = rows_of(i)
            factor = f_ref[here, :]
            square = dot(factor, f_ref[...])
            g_ref[here, :] = square.astype(jnp.bfloat16)
            h_ref[here, :] = (5.0 * factor.astype(jnp.float32) - 4.0 * square).astype(jnp.bfloat16)
            return 0

        lax.fori_loop(0, order // step, second, 0)

        def third(i, _):
            here = rows_of(i)
            a_ref[here, :] = dot(g_ref[here, :], g_ref[...]).astype(jnp.bfloat16)
            return 0

        lax.fori_loop(0, order // step, third, 0)

        def last(i, _):
            here = rows_of(i)
            tail = dot(a_ref[here, :], h_ref[...])
            factor = f_ref[here, :].astype(jnp.float32)
            g_ref[here, :] = ((5.0 * factor - tail) * quarter).astype(jnp.bfloat16)
            return 0

        lax.fori_loop(0, order // step, last, 0)
        rows_ref[...] = g_ref[rows_of(me), :]

    load.wait()

    def line(i, _):
        here = rows_of(i)
        f_ref[here, :] = dot(grad_ref[here, :], g_ref[...]).astype(jnp.bfloat16)
        pltpu.make_async_copy(f_ref.at[here, :], update_hbm.at[here, :], done).start()
        return 0

    lax.fori_loop(0, order // step, line, 0)
    pltpu.make_async_copy(f_ref, update_hbm, done).wait()

    for store in stores:
        store.wait()


def inverse_root(flags, pieces, prev, uppers, grad, part):
    group = pieces.shape[0]
    _, order = grad.shape
    square = pltpu.VMEM((order, order), jnp.bfloat16)
    anywhere = pl.BlockSpec(memory_space=pl.ANY)
    return pl.pallas_call(
        functools.partial(root_kernel, group),
        in_specs=[smem(), vmem(), vmem()] + [anywhere] * 5,
        out_specs=(anywhere, vmem(), anywhere),
        out_shape=(
            jax.ShapeDtypeStruct(part.shape, jnp.float32),
            jax.ShapeDtypeStruct(prev.shape, jnp.bfloat16),
            jax.ShapeDtypeStruct(grad.shape, jnp.bfloat16),
        ),
        input_output_aliases={7: 0},
        scratch_shapes=[square] * 4
        + [
            pltpu.VMEM(grad.shape, jnp.bfloat16),
            pltpu.VMEM((group - 1, B, order), jnp.bfloat16),
            pltpu.VMEM((2 * (group - 1), B, B), jnp.float32),
            pltpu.SemaphoreType.DMA((3 * group - 1,)),
        ],
        compiler_params=params(60),
        cost_estimate=cost(10 * order**3, 8 * MIB),
        name="root",
    )(flags, pieces, prev, *uppers, grad, part)


def step_of(tokens, cotangent, routing, stat_prev, root_prev, owner_map):
    experts = lax.axis_size("expert")
    group = lax.axis_size("group")
    my_expert = lax.axis_index("expert")
    me = lax.axis_index("group").astype(jnp.int32)
    rows, wide = tokens.shape
    order = cotangent.shape[1]
    owners = experts // 4
    live = (jnp.take(owner_map, my_expert) < owners).astype(jnp.int32)
    flags = jnp.stack([me, live])

    def shifted(x, k):
        return lax.ppermute(x, "group", [(g, (g + k) % group) for g in range(group)])

    prev = root_prev[0]
    upper = prev[:B]
    uppers = [shifted(upper, k) for k in range(1, group)]
    sent = dispatch(routing.reshape(1, rows), tokens, cotangent, experts)
    sent = sent.reshape(experts, SLOTS, wide + order)
    got = lax.all_to_all(sent, "expert", 0, 0, tiled=True)
    grad, part = gradient(got.reshape(experts * SLOTS, -1), group, wide, 1.0 / math.sqrt(rows))
    parts = lax.all_to_all(part, "group", 0, 0, tiled=True)
    parts, *uppers = lax.optimization_barrier((parts, *uppers))
    stat_own, send = new_statistic(flags, parts, stat_prev[0], prev, wide * group)
    pieces = lax.all_to_all(send, "group", 0, 0, tiled=True)
    stat, root_rows, update = inverse_root(flags, pieces, prev, uppers, grad, stat_own)
    return stat[None], root_rows[None], update[None]


def solution(mesh):
    in_specs = (
        P("expert", "group"),
        P("expert", None),
        P("expert", None),
        P("expert", "group", None),
        P("expert", "group", None),
        P(),
    )
    out_specs = (P("expert", "group", None), P("expert", "group", None), P("expert", "group", None))
    return jax.shard_map(step_of, mesh=mesh, in_specs=in_specs, out_specs=out_specs, check_vma=False)
```

```python
import functools
import math

import jax
import jax.numpy as jnp
from jax import lax
from jax.experimental import pallas as pl
from jax.experimental.pallas import tpu as pltpu
from jax.sharding import PartitionSpec as P


POWER = 8
KEEP = 0.9
SLOTS = 16
B = 128
HALF = 8
PIECE = 9
MIB = 1024 * 1024


def vmem():
    return pl.BlockSpec(memory_space=pltpu.VMEM)


def smem():
    return pl.BlockSpec(memory_space=pltpu.SMEM)


def params(mib):
    return pltpu.CompilerParams(vmem_limit_bytes=mib * MIB)


def cost(flops, nbytes):
    return pl.CostEstimate(flops=int(flops), bytes_accessed=int(nbytes), transcendentals=0)


def outer(a, b):
    return lax.dot_general(a, b, (((0,), (0,)), ((), ())), preferred_element_type=jnp.float32)


def dot(a, b):
    return jnp.dot(a, b, preferred_element_type=jnp.float32)


def ones_where(mask):
    return jnp.where(mask, 1.0, 0.0).astype(jnp.bfloat16)


def dispatch_kernel(experts, route_hbm, tok_hbm, sig_hbm, out_ref, route_ref, slot_ref, tok_ref, sig_ref, sems):
    tokens = route_ref.shape[1]
    wide = tok_ref.shape[1]
    rows = out_ref.shape[0]

    @pl.when(pl.program_id(0) == 0)
    def _():
        copies = [
            pltpu.make_async_copy(route_hbm, route_ref, sems.at[0]),
            pltpu.make_async_copy(tok_hbm, tok_ref, sems.at[1]),
            pltpu.make_async_copy(sig_hbm, sig_ref, sems.at[2]),
        ]
        for copy in copies:
            copy.start()
        before = lax.broadcasted_iota(jnp.int32, (tokens, tokens), 0) < lax.broadcasted_iota(
            jnp.int32, (tokens, tokens), 1
        )
        before = ones_where(before)
        copies[0].wait()
        route = route_ref[...]
        hot = lax.broadcasted_iota(jnp.int32, (experts, tokens), 0) == route
        earlier = dot(ones_where(hot), before)
        position = jnp.sum(jnp.where(hot, earlier, 0.0), axis=0, keepdims=True)
        slot_ref[...] = route * SLOTS + position.astype(jnp.int32)
        copies[1].wait()
        copies[2].wait()

    at = lax.broadcasted_iota(jnp.int32, (rows, tokens), 0) + pl.program_id(0) * rows
    pick = ones_where(at == slot_ref[...])
    out_ref[:, :wide] = dot(pick, tok_ref[...]).astype(jnp.bfloat16)
    out_ref[:, wide:] = dot(pick, sig_ref[...]).astype(jnp.bfloat16)


def dispatch(route, tokens, signal, experts):
    count, wide = tokens.shape
    hidden = signal.shape[1]
    total, rows = experts * SLOTS, B
    return pl.pallas_call(
        functools.partial(dispatch_kernel, experts),
        grid=(total // rows,),
        in_specs=[pl.BlockSpec(memory_space=pl.ANY)] * 3,
        out_specs=pl.BlockSpec((rows, wide + hidden), lambda i: (i, 0)),
        out_shape=jax.ShapeDtypeStruct((total, wide + hidden), jnp.bfloat16),
        scratch_shapes=[
            pltpu.VMEM((1, count), jnp.int32),
            pltpu.VMEM((1, count), jnp.int32),
            pltpu.VMEM((count, wide), jnp.bfloat16),
            pltpu.VMEM((count, hidden), jnp.bfloat16),
            pltpu.SemaphoreType.DMA((3,)),
        ],
        compiler_params=params(60),
        cost_estimate=cost(2 * total * count * (wide + hidden), 6 * MIB),
        name="dispatch",
    )(route, tokens, signal)


def owned_blocks(d, group):
    found = [(d, d, 0, 0), (d, d, 0, 1), (d, d, 1, 1)]
    for h in range(group):
        if h > d:
            found += [(d, h, 0, 0), (d, h, 0, 1)]
        if h < d:
            found += [(h, d, 1, 0), (h, d, 1, 1)]
    return found


def gradient_kernel(group, scale, x_ref, grad_hbm, part_hbm, grad_ref, part_ref, sems):
    wide = grad_ref.shape[0]
    step = 2 * B
    lines = wide // step
    stores = []
    for r in range(lines):
        at = slice(r * step, (r + 1) * step)
        grad_ref[at, :] = (outer(x_ref[:, at], x_ref[:, wide:]) * scale).astype(jnp.bfloat16)
        stores.append(pltpu.make_async_copy(grad_ref.at[at, :], grad_hbm.at[at, :], sems.at[r]))
        stores[-1].start()
    place = {}
    for d in range(group):
        for k, name in enumerate(owned_blocks(d, group)):
            place[name] = (d, k)
    last = {d: max((p, q) for (p, q, _, _) in owned_blocks(d, group)) for d in range(group)}
    for p in range(group):
        for q in range(p, group):
            gram = outer(
                grad_ref[:, p * step : (p + 1) * step], grad_ref[:, q * step : (q + 1) * step]
            ).astype(jnp.bfloat16)
            for i in range(2):
                for j in range(2):
                    if (p, q, i, j) in place:
                        d, k = place[(p, q, i, j)]
                        part_ref[d, k * B : (k + 1) * B, :] = gram[
                            i * B : (i + 1) * B, j * B : (j + 1) * B
                        ]
            for d in range(group):
                if last[d] == (p, q):
                    stores.append(pltpu.make_async_copy(part_ref.at[d], part_hbm.at[d], sems.at[lines + d]))
                    stores[-1].start()
    for store in stores:
        store.wait()


def gradient(x, group, wide, scale):
    total, both = x.shape
    hidden = both - wide
    part = (group, PIECE * B, B)
    return pl.pallas_call(
        functools.partial(gradient_kernel, group, scale),
        in_specs=[vmem()],
        out_specs=(pl.BlockSpec(memory_space=pl.ANY),) * 2,
        out_shape=(
            jax.ShapeDtypeStruct((wide, hidden), jnp.bfloat16),
            jax.ShapeDtypeStruct(part, jnp.bfloat16),
        ),
        scratch_shapes=[
            pltpu.VMEM((wide, hidden), jnp.bfloat16),
            pltpu.VMEM(part, jnp.bfloat16),
            pltpu.SemaphoreType.DMA((wide // (2 * B) + group,)),
        ],
        compiler_params=params(16),
        cost_estimate=cost(2 * wide * hidden * (total + hidden), 10 * MIB),
        name="gradient",
    )(x)


def statistic_kernel(
    group, full, flags_ref, parts_ref, prev_ref, root_ref, stat_hbm, send_ref, stat_ref, own_ref, sem
):
    me, live = flags_ref[0], flags_ref[1]

    def gram(k):
        total = parts_ref[0, k * B : (k + 1) * B, :].astype(jnp.float32)
        for s in range(1, group):
            total += parts_ref[s, k * B : (k + 1) * B, :].astype(jnp.float32)
        return total

    def put(k, block, row, col):
        at = (slice(row, row + B), pl.ds(pl.multiple_of(col, B), B))
        new = KEEP * prev_ref[at] + (1.0 - KEEP) * block / full
        stat_ref[at] = new
        own_ref[k * B : (k + 1) * B, :] = new.astype(jnp.bfloat16)

    mine = pl.multiple_of(me * 2 * B, 2 * B)
    put(0, gram(0), 0, mine)
    put(1, gram(1), 0, mine + B)
    put(2, gram(2), B, mine + B)
    for j in range(group - 1):
        k = 3 + 2 * j

        @pl.when(j >= me)
        def _():
            col = (j + 1) * 2 * B
            put(k, gram(k), 0, col)
            put(k + 1, gram(k + 1), 0, col + B)

        @pl.when(j < me)
        def _():
            col = j * 2 * B + B
            put(k, gram(k).T, 0, col)
            put(k + 1, gram(k + 1).T, B, col)

    stat_ref[B:, pl.ds(mine, B)] = stat_ref[:B, pl.ds(mine + B, B)].T
    store = pltpu.make_async_copy(stat_ref, stat_hbm, sem)
    store.start()

    @pl.when(live != 0)
    def _():
        for t in range(group):
            send_ref[t, : PIECE * B, :] = own_ref[...]

    @pl.when(live == 0)
    def _():
        for t in range(group):
            for c in range(HALF):
                send_ref[t, (2 + c) * B : (3 + c) * B, :] = root_ref[B:, c * B : (c + 1) * B]
            send_ref[t, : 2 * B, :] = own_ref[pl.ds(shared(me, t), 2 * B), :]

    store.wait()


def shared(s, t):
    other = jnp.where(t > s, t - 1, jnp.minimum(t, PIECE // 2 - 2))
    return pl.multiple_of((3 + 2 * other) * B, B)


def new_statistic(flags, parts, prev, root, full):
    group = parts.shape[0]
    return pl.pallas_call(
        functools.partial(statistic_kernel, group, float(full)),
        in_specs=[smem(), vmem(), vmem(), vmem()],
        out_specs=(pl.BlockSpec(memory_space=pl.ANY), vmem()),
        out_shape=(
            jax.ShapeDtypeStruct(prev.shape, jnp.float32),
            jax.ShapeDtypeStruct((group, (2 + HALF) * B, B), jnp.bfloat16),
        ),
        scratch_shapes=[
            pltpu.VMEM(prev.shape, jnp.float32),
            pltpu.VMEM((PIECE * B, B), jnp.bfloat16),
            pltpu.SemaphoreType.DMA,
        ],
        compiler_params=params(8),
        cost_estimate=cost(4 * prev.size, 4 * MIB),
        name="statistic",
    )(flags, parts, prev, root)


def root_kernel(
    group,
    flags_ref,
    pieces_ref,
    prev_ref,
    first_ref,
    second_ref,
    third_ref,
    grad_hbm,
    part_hbm,
    stat_hbm,
    rows_hbm,
    update_hbm,
    a_ref,
    f_ref,
    g_ref,
    h_ref,
    grad_ref,
    mirror_ref,
    sems,
):
    me, live = flags_ref[0], flags_ref[1]
    order = a_ref.shape[0]
    step = 2 * B
    done = sems.at[2 * group - 2]
    load = pltpu.make_async_copy(grad_hbm, grad_ref, sems.at[2 * group - 1])
    rows_sem = sems.at[2 * group]
    load.start()

    def mirrored(j):
        s = jnp.where(j < me, j, j + 1)
        start = jnp.where(live != 0, shared(s, me), 0)
        col = pl.multiple_of(s * step, step)
        found = []
        for k in range(2):
            at = pl.ds(pl.multiple_of(start + k * B, B), B)
            mirror_ref[2 * j + k] = pieces_ref[s, at, :].astype(jnp.float32).T
            row = jnp.where(j < me, k * B, B)
            place = col + jnp.where(j < me, 0, k * B)
            target = stat_hbm.at[pl.ds(pl.multiple_of(row, B), B), pl.ds(pl.multiple_of(place, B), B)]
            found.append(pltpu.make_async_copy(mirror_ref.at[2 * j + k], target, sems.at[2 * j + k]))
        return found

    stores = []
    for j in range(group - 1):
        stores += mirrored(j)
        stores[-2].start()
        stores[-1].start()

    def rows_of(i, count=step):
        return pl.ds(pl.multiple_of(i * step, step), count)

    @pl.when(live == 0)
    def _():
        pltpu.make_async_copy(prev_ref, rows_hbm, rows_sem).start()
        for s in range(group):
            for c in range(HALF):
                g_ref[s * step + B : (s + 1) * step, c * B : (c + 1) * B] = pieces_ref[
                    s, (2 + c) * B : (3 + c) * B, :
                ]
        g_ref[rows_of(me, B), :] = prev_ref[:B, :]
        for k, upper_ref in enumerate((first_ref, second_ref, third_ref)):
            g_ref[rows_of(lax.rem(me - k - 1 + group, group), B), :] = upper_ref[...]

    @pl.when(live != 0)
    def _():
        def fill(block, row, col, mirror=True):
            a_ref[row : row + B, col : col + B] = block
            if mirror:
                a_ref[col : col + B, row : row + B] = block.T

        for s in range(group):
            at = s * step
            block = [pieces_ref[s, k * B : (k + 1) * B, :] for k in range(PIECE)]
            fill(block[0], at, at, False)
            fill(block[1], at, at + B)
            fill(block[2], at + B, at + B, False)
            k = 3
            for h in range(group):
                if h > s:
                    fill(block[k], at, h * step)
                    fill(block[k + 1], at, h * step + B)
                if h < s:
                    fill(block[k], at, h * step + B)
                    fill(block[k + 1], at + B, h * step + B)
                if h != s:
                    k += 2

        def power(_, carry):
            vector, _ = carry
            image = dot(vector.astype(jnp.bfloat16), a_ref[...])
            length = jnp.sqrt(jnp.sum(image * image, axis=1, keepdims=True))
            return image / length, length

        vector = jnp.full((16, order), 1.0 / math.sqrt(order), jnp.float32)
        length = jnp.ones((16, 1), jnp.float32)
        _, length = lax.fori_loop(0, POWER, power, (vector, length))
        scaling = 2.5 / length[:1, :1]
        quarter = jnp.sqrt(jnp.sqrt(scaling)) * 0.25

        def first(i, _):
            here = rows_of(i)
            line = lax.broadcasted_iota(jnp.int32, (step, order), 0) + i * step
            eye = line == lax.broadcasted_iota(jnp.int32, (step, order), 1)
            moment = scaling * a_ref[here, :].astype(jnp.float32)
            f_ref[here, :] = ((jnp.where(eye, 5.0, 0.0) - moment) * 0.25).astype(jnp.bfloat16)
            return 0

        lax.fori_loop(0, order // step, first, 0)

        def second(i, _):
            here = rows_of(i)
            factor = f_ref[here, :]
            square = dot(factor, f_ref[...])
            g_ref[here, :] = square.astype(jnp.bfloat16)
            h_ref[here, :] = (5.0 * factor.astype(jnp.float32) - 4.0 * square).astype(jnp.bfloat16)
            return 0

        lax.fori_loop(0, order // step, second, 0)

        def third(i, _):
            here = rows_of(i)
            a_ref[here, :] = dot(g_ref[here, :], g_ref[...]).astype(jnp.bfloat16)
            return 0

        lax.fori_loop(0, order // step, third, 0)

        def last(i, _):
            here = rows_of(i)
            tail = dot(a_ref[here, :], h_ref[...])
            factor = f_ref[here, :].astype(jnp.float32)
            g_ref[here, :] = ((5.0 * factor - tail) * quarter).astype(jnp.bfloat16)
            return 0

        lax.fori_loop(0, order // step, last, 0)
        pltpu.make_async_copy(g_ref.at[rows_of(me), :], rows_hbm, rows_sem).start()

    load.wait()

    def line(i, _):
        here = rows_of(i)
        f_ref[here, :] = dot(grad_ref[here, :], g_ref[...]).astype(jnp.bfloat16)
        pltpu.make_async_copy(f_ref.at[here, :], update_hbm.at[here, :], done).start()
        return 0

    lax.fori_loop(0, order // step, line, 0)
    pltpu.make_async_copy(f_ref, update_hbm, done).wait()
    pltpu.make_async_copy(prev_ref, rows_hbm, rows_sem).wait()

    for store in stores:
        store.wait()


def inverse_root(flags, pieces, prev, uppers, grad, part):
    group = pieces.shape[0]
    _, order = grad.shape
    square = pltpu.VMEM((order, order), jnp.bfloat16)
    anywhere = pl.BlockSpec(memory_space=pl.ANY)
    return pl.pallas_call(
        functools.partial(root_kernel, group),
        in_specs=[smem()] + [vmem()] * (1 + group) + [anywhere] * 2,
        out_specs=(anywhere, anywhere, anywhere),
        out_shape=(
            jax.ShapeDtypeStruct(part.shape, jnp.float32),
            jax.ShapeDtypeStruct(prev.shape, jnp.bfloat16),
            jax.ShapeDtypeStruct(grad.shape, jnp.bfloat16),
        ),
        input_output_aliases={7: 0, 6: 2},
        scratch_shapes=[square] * 4
        + [
            pltpu.VMEM(grad.shape, jnp.bfloat16),
            pltpu.VMEM((2 * (group - 1), B, B), jnp.float32),
            pltpu.SemaphoreType.DMA((2 * group + 1,)),
        ],
        compiler_params=params(20),
        cost_estimate=cost(10 * order**3, 8 * MIB),
        name="root",
    )(flags, pieces, prev, *uppers, grad, part)


def step_of(tokens, cotangent, routing, stat_prev, root_prev, owner_map):
    experts = lax.axis_size("expert")
    group = lax.axis_size("group")
    my_expert = lax.axis_index("expert")
    me = lax.axis_index("group").astype(jnp.int32)
    rows, wide = tokens.shape
    order = cotangent.shape[1]
    owners = experts // 4
    live = (jnp.take(owner_map, my_expert) < owners).astype(jnp.int32)
    flags = jnp.stack([me, live])

    def shifted(x, k):
        return lax.ppermute(x, "group", [(g, (g + k) % group) for g in range(group)])

    prev = root_prev[0]
    upper = prev[:B]
    uppers = [shifted(upper, k) for k in range(1, group)]
    sent = dispatch(routing.reshape(1, rows), tokens, cotangent, experts)
    sent = sent.reshape(experts, SLOTS, wide + order)
    got = lax.all_to_all(sent, "expert", 0, 0, tiled=True)
    grad, part = gradient(got.reshape(experts * SLOTS, -1), group, wide, 1.0 / math.sqrt(rows))
    parts = lax.all_to_all(part, "group", 0, 0, tiled=True)
    parts, *uppers = lax.optimization_barrier((parts, *uppers))
    stat_own, send = new_statistic(flags, parts, stat_prev[0], prev, wide * group)
    pieces = lax.all_to_all(send, "group", 0, 0, tiled=True)
    stat, root_rows, update = inverse_root(flags, pieces, prev, uppers, grad, stat_own)
    return stat[None], root_rows[None], update[None]


def solution(mesh):
    in_specs = (
        P("expert", "group"),
        P("expert", None),
        P("expert", None),
        P("expert", "group", None),
        P("expert", "group", None),
        P(),
    )
    out_specs = (P("expert", "group", None), P("expert", "group", None), P("expert", "group", None))
    return jax.shard_map(step_of, mesh=mesh, in_specs=in_specs, out_specs=out_specs, check_vma=False)
```

```python
import functools
import math

import jax
import jax.numpy as jnp
from jax import lax
from jax.experimental import pallas as pl
from jax.experimental.pallas import tpu as pltpu
from jax.sharding import PartitionSpec as P


POWER = 8
KEEP = 0.9
SLOTS = 16
B = 128
PIECE = 9
REST = 112
MIB = 1024 * 1024


def vmem():
    return pl.BlockSpec(memory_space=pltpu.VMEM)


def smem():
    return pl.BlockSpec(memory_space=pltpu.SMEM)


def params(mib):
    return pltpu.CompilerParams(vmem_limit_bytes=mib * MIB)


def cost(flops, nbytes):
    return pl.CostEstimate(flops=int(flops), bytes_accessed=int(nbytes), transcendentals=0)


def outer(a, b):
    return lax.dot_general(a, b, (((0,), (0,)), ((), ())), preferred_element_type=jnp.float32)


def dot(a, b):
    return jnp.dot(a, b, preferred_element_type=jnp.float32)


def ones_where(mask):
    return jnp.where(mask, 1.0, 0.0).astype(jnp.bfloat16)


def dispatch_kernel(experts, route_hbm, tok_hbm, sig_hbm, out_hbm, route_ref, tok_ref, sig_ref, out_ref, sems):
    tokens = route_ref.shape[1]
    wide = tok_ref.shape[1]
    rows = 2 * B
    loads = [
        pltpu.make_async_copy(route_hbm, route_ref, sems.at[0]),
        pltpu.make_async_copy(tok_hbm, tok_ref, sems.at[1]),
        pltpu.make_async_copy(sig_hbm, sig_ref, sems.at[2]),
    ]
    for load in loads:
        load.start()
    before = lax.broadcasted_iota(jnp.int32, (tokens, tokens), 0) < lax.broadcasted_iota(
        jnp.int32, (tokens, tokens), 1
    )
    before = ones_where(before)
    loads[0].wait()
    route = route_ref[...]
    hot = lax.broadcasted_iota(jnp.int32, (experts, tokens), 0) == route
    earlier = dot(ones_where(hot), before)
    position = jnp.sum(jnp.where(hot, earlier, 0.0), axis=0, keepdims=True)
    slot = route * SLOTS + position.astype(jnp.int32)
    line = lax.broadcasted_iota(jnp.int32, (rows, tokens), 0)
    stores = []
    for part, (source, col) in enumerate(((tok_ref, 0), (sig_ref, wide))):
        loads[1 + part].wait()
        for start in range(0, out_ref.shape[0], rows):
            at = (slice(start, start + rows), slice(col, col + source.shape[1]))
            pick = ones_where(line + start == slot)
            out_ref[at] = dot(pick, source[...]).astype(jnp.bfloat16)
            stores.append(pltpu.make_async_copy(out_ref.at[at], out_hbm.at[at], sems.at[3 + len(stores)]))
            stores[-1].start()
    for store in stores:
        store.wait()


def dispatch(route, tokens, signal, experts):
    count, wide = tokens.shape
    hidden = signal.shape[1]
    total = experts * SLOTS
    anywhere = pl.BlockSpec(memory_space=pl.ANY)
    return pl.pallas_call(
        functools.partial(dispatch_kernel, experts),
        in_specs=[anywhere] * 3,
        out_specs=anywhere,
        out_shape=jax.ShapeDtypeStruct((total, wide + hidden), jnp.bfloat16),
        scratch_shapes=[
            pltpu.VMEM((1, count), jnp.int32),
            pltpu.VMEM((count, wide), jnp.bfloat16),
            pltpu.VMEM((count, hidden), jnp.bfloat16),
            pltpu.VMEM((total, wide + hidden), jnp.bfloat16),
            pltpu.SemaphoreType.DMA((3 + 2 * (total // (2 * B)),)),
        ],
        compiler_params=params(60),
        cost_estimate=cost(2 * total * count * (wide + hidden), 6 * MIB),
        name="dispatch",
    )(route, tokens, signal)


def owned_blocks(d, group):
    found = [(d, d, 0, 0), (d, d, 0, 1), (d, d, 1, 1)]
    for h in range(group):
        if h > d:
            found += [(d, h, 0, 0), (d, h, 0, 1)]
        if h < d:
            found += [(h, d, 1, 0), (h, d, 1, 1)]
    return found


def gradient_kernel(group, scale, x_ref, grad_hbm, part_hbm, grad_ref, part_ref, sems):
    wide = grad_ref.shape[0]
    step = 2 * B
    lines = wide // step
    stores = []
    for r in range(lines):
        at = slice(r * step, (r + 1) * step)
        grad_ref[at, :] = (outer(x_ref[:, at], x_ref[:, wide:]) * scale).astype(jnp.bfloat16)
        stores.append(pltpu.make_async_copy(grad_ref.at[at, :], grad_hbm.at[at, :], sems.at[r]))
        stores[-1].start()
    place = {}
    for d in range(group):
        for k, name in enumerate(owned_blocks(d, group)):
            place[name] = (d, k)
    last = {d: max((p, q) for (p, q, _, _) in owned_blocks(d, group)) for d in range(group)}
    for p in range(group):
        for q in range(p, group):
            gram = outer(
                grad_ref[:, p * step : (p + 1) * step], grad_ref[:, q * step : (q + 1) * step]
            ).astype(jnp.bfloat16)
            for i in range(2):
                for j in range(2):
                    if (p, q, i, j) in place:
                        d, k = place[(p, q, i, j)]
                        part_ref[d, k * B : (k + 1) * B, :] = gram[
                            i * B : (i + 1) * B, j * B : (j + 1) * B
                        ]
            for d in range(group):
                if last[d] == (p, q):
                    stores.append(pltpu.make_async_copy(part_ref.at[d], part_hbm.at[d], sems.at[lines + d]))
                    stores[-1].start()
    for store in stores:
        store.wait()


def gradient(x, group, wide, scale):
    total, both = x.shape
    hidden = both - wide
    part = (group, PIECE * B, B)
    return pl.pallas_call(
        functools.partial(gradient_kernel, group, scale),
        in_specs=[vmem()],
        out_specs=(pl.BlockSpec(memory_space=pl.ANY),) * 2,
        out_shape=(
            jax.ShapeDtypeStruct((wide, hidden), jnp.bfloat16),
            jax.ShapeDtypeStruct(part, jnp.bfloat16),
        ),
        scratch_shapes=[
            pltpu.VMEM((wide, hidden), jnp.bfloat16),
            pltpu.VMEM(part, jnp.bfloat16),
            pltpu.SemaphoreType.DMA((wide // (2 * B) + group,)),
        ],
        compiler_params=params(16),
        cost_estimate=cost(2 * wide * hidden * (total + hidden), 10 * MIB),
        name="gradient",
    )(x)


def statistic_kernel(
    group, full, flags_ref, parts_ref, prev_ref, root_ref, stat_hbm, send_ref, stat_ref, own_ref, sem
):
    me, live = flags_ref[0], flags_ref[1]

    def gram(k):
        total = parts_ref[0, k * B : (k + 1) * B, :].astype(jnp.float32)
        for s in range(1, group):
            total += parts_ref[s, k * B : (k + 1) * B, :].astype(jnp.float32)
        return total

    def put(k, block, row, col):
        at = (slice(row, row + B), pl.ds(pl.multiple_of(col, B), B))
        new = KEEP * prev_ref[at] + (1.0 - KEEP) * block / full
        stat_ref[at] = new
        own_ref[k * B : (k + 1) * B, :] = new.astype(jnp.bfloat16)

    mine = pl.multiple_of(me * 2 * B, 2 * B)
    put(0, gram(0), 0, mine)
    put(1, gram(1), 0, mine + B)
    put(2, gram(2), B, mine + B)
    for j in range(group - 1):
        k = 3 + 2 * j

        @pl.when(j >= me)
        def _():
            col = (j + 1) * 2 * B
            put(k, gram(k), 0, col)
            put(k + 1, gram(k + 1), 0, col + B)

        @pl.when(j < me)
        def _():
            col = j * 2 * B + B
            put(k, gram(k).T, 0, col)
            put(k + 1, gram(k + 1).T, B, col)

    stat_ref[B:, pl.ds(mine, B)] = stat_ref[:B, pl.ds(mine + B, B)].T
    store = pltpu.make_async_copy(stat_ref, stat_hbm, sem)
    store.start()

    @pl.when(live != 0)
    def _():
        for t in range(group):
            send_ref[t] = own_ref[...]

    @pl.when(live == 0)
    def _():
        for t in range(group):
            for c in range(root_ref.shape[1] // B):
                at = slice(2 * B + c * REST, 2 * B + (c + 1) * REST)
                send_ref[t, at, :] = root_ref[-REST:, c * B : (c + 1) * B]
            send_ref[t, : 2 * B, :] = own_ref[pl.ds(shared(me, t), 2 * B), :]

    store.wait()


def shared(s, t):
    other = jnp.where(t > s, t - 1, jnp.minimum(t, PIECE // 2 - 2))
    return pl.multiple_of((3 + 2 * other) * B, B)


def new_statistic(flags, parts, prev, root, full):
    group = parts.shape[0]
    return pl.pallas_call(
        functools.partial(statistic_kernel, group, float(full)),
        in_specs=[smem(), vmem(), vmem(), vmem()],
        out_specs=(pl.BlockSpec(memory_space=pl.ANY), vmem()),
        out_shape=(
            jax.ShapeDtypeStruct(prev.shape, jnp.float32),
            jax.ShapeDtypeStruct((group, PIECE * B, B), jnp.bfloat16),
        ),
        scratch_shapes=[
            pltpu.VMEM(prev.shape, jnp.float32),
            pltpu.VMEM((PIECE * B, B), jnp.bfloat16),
            pltpu.SemaphoreType.DMA,
        ],
        compiler_params=params(8),
        cost_estimate=cost(4 * prev.size, 4 * MIB),
        name="statistic",
    )(flags, parts, prev, root)


def root_kernel(
    group,
    flags_ref,
    pieces_ref,
    prev_ref,
    first_ref,
    second_ref,
    third_ref,
    grad_hbm,
    part_hbm,
    stat_hbm,
    rows_hbm,
    update_hbm,
    a_ref,
    f_ref,
    g_ref,
    h_ref,
    s_ref,
    grad_ref,
    mirror_ref,
    sems,
):
    me, live = flags_ref[0], flags_ref[1]
    order = a_ref.shape[0]
    step = 2 * B
    done = sems.at[2 * group - 2]
    load = pltpu.make_async_copy(grad_hbm, grad_ref, sems.at[2 * group - 1])
    rows_sem = sems.at[2 * group]
    load.start()

    def mirrored(j):
        s = jnp.where(j < me, j, j + 1)
        start = jnp.where(live != 0, shared(s, me), 0)
        col = pl.multiple_of(s * step, step)
        found = []
        for k in range(2):
            at = pl.ds(pl.multiple_of(start + k * B, B), B)
            mirror_ref[2 * j + k] = pieces_ref[s, at, :].astype(jnp.float32).T
            row = jnp.where(j < me, k * B, B)
            place = col + jnp.where(j < me, 0, k * B)
            target = stat_hbm.at[pl.ds(pl.multiple_of(row, B), B), pl.ds(pl.multiple_of(place, B), B)]
            found.append(pltpu.make_async_copy(mirror_ref.at[2 * j + k], target, sems.at[2 * j + k]))
        return found

    stores = []
    for j in range(group - 1):
        stores += mirrored(j)
        stores[-2].start()
        stores[-1].start()

    def rows_of(i, count=step):
        return pl.ds(pl.multiple_of(i * step, step), count)

    @pl.when(live == 0)
    def _():
        pltpu.make_async_copy(prev_ref, rows_hbm, rows_sem).start()
        for s in range(group):
            for c in range(order // B):
                at = slice(2 * B + c * REST, 2 * B + (c + 1) * REST)
                g_ref[(s + 1) * step - REST : (s + 1) * step, c * B : (c + 1) * B] = pieces_ref[s, at, :]
        g_ref[rows_of(me, step - REST), :] = prev_ref[: step - REST, :]
        for k, upper_ref in enumerate((first_ref, second_ref, third_ref)):
            g_ref[rows_of(lax.rem(me - k - 1 + group, group), step - REST), :] = upper_ref[...]

    @pl.when(live != 0)
    def _():
        def fill(block, row, col, mirror=True):
            a_ref[row : row + B, col : col + B] = block
            if mirror:
                a_ref[col : col + B, row : row + B] = block.T

        for s in range(group):
            at = s * step
            block = [pieces_ref[s, k * B : (k + 1) * B, :] for k in range(PIECE)]
            fill(block[0], at, at, False)
            fill(block[1], at, at + B)
            fill(block[2], at + B, at + B, False)
            k = 3
            for h in range(group):
                if h > s:
                    fill(block[k], at, h * step)
                    fill(block[k + 1], at, h * step + B)
                if h < s:
                    fill(block[k], at, h * step + B)
                    fill(block[k + 1], at + B, h * step + B)
                if h != s:
                    k += 2

        lines = range(order // step)
        row = lax.broadcasted_iota(jnp.int32, (step, step), 0)
        eye = row == lax.broadcasted_iota(jnp.int32, (step, step), 1)

        def both(ref, i, j, block):
            ref[i * step : (i + 1) * step, j * step : (j + 1) * step] = block
            if i != j:
                ref[j * step : (j + 1) * step, i * step : (i + 1) * step] = block.T

        def piece(ref, i, j):
            return ref[i * step : (i + 1) * step, j * step : (j + 1) * step]

        def upper_product(left, right, use):
            for i in lines:
                found = dot(left[i * step : (i + 1) * step, :], right[:, i * step :])
                for j in lines[i:]:
                    use(i, j, found[:, (j - i) * step : (j - i + 1) * step])

        largest = jnp.zeros((1, step), jnp.float32)
        for i in lines:
            diagonal = jnp.where(eye, piece(a_ref, i, i).astype(jnp.float32), 0.0)
            largest = jnp.maximum(largest, jnp.max(diagonal, axis=0, keepdims=True))
        unit = 1.0 / jnp.max(largest, axis=1, keepdims=True)

        def squared(i, j, block):
            s_ref[i * step : (i + 1) * step, j * step : (j + 1) * step] = block
            both(g_ref, i, j, (block * unit * unit).astype(jnp.bfloat16))

        upper_product(a_ref, a_ref, squared)

        def applied(vector, matrix_ref):
            image = dot(vector.astype(jnp.bfloat16), matrix_ref[...])
            length = jnp.sqrt(jnp.sum(image * image, axis=1, keepdims=True))
            return image / length, length

        vector = jnp.full((16, order), 1.0 / math.sqrt(order), jnp.float32)
        vector = lax.fori_loop(0, POWER // 2 - 1, lambda _, v: applied(v, g_ref)[0], vector)
        vector, _ = applied(vector, a_ref)
        _, length = applied(vector, a_ref)
        scaling = 2.5 / length[:1, :1]
        quarter = jnp.sqrt(jnp.sqrt(scaling)) * 0.25

        for i in lines:
            for j in lines[i:]:
                moment = scaling * piece(a_ref, i, j).astype(jnp.float32)
                twice = scaling * (scaling * piece(s_ref, i, j))
                square = twice - 10.0 * moment
                if i == j:
                    square += jnp.where(eye, 25.0, 0.0)
                both(g_ref, i, j, (square * 0.0625).astype(jnp.bfloat16))
                both(h_ref, i, j, ((5.0 * moment - twice) * 0.25).astype(jnp.bfloat16))

        upper_product(g_ref, g_ref, lambda i, j, block: both(f_ref, i, j, block.astype(jnp.bfloat16)))

        def root(i, j, tail):
            factor = -1.25 * scaling * piece(a_ref, i, j).astype(jnp.float32)
            if i == j:
                factor += jnp.where(eye, 6.25, 0.0)
            both(g_ref, i, j, ((factor - tail) * quarter).astype(jnp.bfloat16))

        upper_product(f_ref, h_ref, root)
        pltpu.make_async_copy(g_ref.at[rows_of(me), :], rows_hbm, rows_sem).start()

    load.wait()

    def line(i, _):
        here = rows_of(i)
        f_ref[here, :] = dot(grad_ref[here, :], g_ref[...]).astype(jnp.bfloat16)
        pltpu.make_async_copy(f_ref.at[here, :], update_hbm.at[here, :], done).start()
        return 0

    lax.fori_loop(0, order // step, line, 0)
    pltpu.make_async_copy(f_ref, update_hbm, done).wait()
    pltpu.make_async_copy(prev_ref, rows_hbm, rows_sem).wait()

    for store in stores:
        store.wait()


def inverse_root(flags, pieces, prev, uppers, grad, part):
    group = pieces.shape[0]
    _, order = grad.shape
    square = pltpu.VMEM((order, order), jnp.bfloat16)
    anywhere = pl.BlockSpec(memory_space=pl.ANY)
    return pl.pallas_call(
        functools.partial(root_kernel, group),
        in_specs=[smem()] + [vmem()] * (1 + group) + [anywhere] * 2,
        out_specs=(anywhere, anywhere, anywhere),
        out_shape=(
            jax.ShapeDtypeStruct(part.shape, jnp.float32),
            jax.ShapeDtypeStruct(prev.shape, jnp.bfloat16),
            jax.ShapeDtypeStruct(grad.shape, jnp.bfloat16),
        ),
        input_output_aliases={7: 0, 6: 2},
        scratch_shapes=[square] * 4
        + [
            pltpu.VMEM((order, order), jnp.float32),
            pltpu.VMEM(grad.shape, jnp.bfloat16),
            pltpu.VMEM((2 * (group - 1), B, B), jnp.float32),
            pltpu.SemaphoreType.DMA((2 * group + 1,)),
        ],
        compiler_params=params(26),
        cost_estimate=cost(10 * order**3, 8 * MIB),
        name="root",
    )(flags, pieces, prev, *uppers, grad, part)


def step_of(tokens, cotangent, routing, stat_prev, root_prev, owner_map):
    experts = lax.axis_size("expert")
    group = lax.axis_size("group")
    my_expert = lax.axis_index("expert")
    me = lax.axis_index("group").astype(jnp.int32)
    rows, wide = tokens.shape
    order = cotangent.shape[1]
    owners = experts // 4
    live = (jnp.take(owner_map, my_expert) < owners).astype(jnp.int32)
    flags = jnp.stack([me, live])

    def shifted(x, k):
        return lax.ppermute(x, "group", [(g, (g + k) % group) for g in range(group)])

    prev = root_prev[0]
    upper = prev[: prev.shape[0] - REST]
    uppers = [shifted(upper, k) for k in range(1, group)]
    sent = dispatch(routing.reshape(1, rows), tokens, cotangent, experts)
    sent = sent.reshape(experts, SLOTS, wide + order)
    got = lax.all_to_all(sent, "expert", 0, 0, tiled=True)
    grad, part = gradient(got.reshape(experts * SLOTS, -1), group, wide, 1.0 / math.sqrt(rows))
    parts = lax.all_to_all(part, "group", 0, 0, tiled=True)
    parts, *uppers = lax.optimization_barrier((parts, *uppers))
    stat_own, send = new_statistic(flags, parts, stat_prev[0], prev, wide * group)
    pieces = lax.all_to_all(send, "group", 0, 0, tiled=True)
    stat, root_rows, update = inverse_root(flags, pieces, prev, uppers, grad, stat_own)
    return stat[None], root_rows[None], update[None]


def solution(mesh):
    in_specs = (
        P("expert", "group"),
        P("expert", None),
        P("expert", None),
        P("expert", "group", None),
        P("expert", "group", None),
        P(),
    )
    out_specs = (P("expert", "group", None), P("expert", "group", None), P("expert", "group", None))
    return jax.shard_map(step_of, mesh=mesh, in_specs=in_specs, out_specs=out_specs, check_vma=False)
```

```python
import functools
import math

import jax
import jax.numpy as jnp
from jax import lax
from jax.experimental import pallas as pl
from jax.experimental.pallas import tpu as pltpu
from jax.sharding import PartitionSpec as P


POWER = 8
KEEP = 0.9
SLOTS = 16
B = 128
PIECE = 9
REST = 112
MIB = 1024 * 1024


def vmem():
    return pl.BlockSpec(memory_space=pltpu.VMEM)


def smem():
    return pl.BlockSpec(memory_space=pltpu.SMEM)


def params(mib):
    return pltpu.CompilerParams(vmem_limit_bytes=mib * MIB)


def cost(flops, nbytes):
    return pl.CostEstimate(flops=int(flops), bytes_accessed=int(nbytes), transcendentals=0)


def outer(a, b):
    return lax.dot_general(a, b, (((0,), (0,)), ((), ())), preferred_element_type=jnp.float32)


def dot(a, b):
    return jnp.dot(a, b, preferred_element_type=jnp.float32)


def ones_where(mask):
    return jnp.where(mask, 1.0, 0.0).astype(jnp.bfloat16)


def dispatch_kernel(experts, route_hbm, tok_hbm, sig_hbm, out_hbm, route_ref, tok_ref, sig_ref, out_ref, sems):
    tokens = route_ref.shape[1]
    wide = tok_ref.shape[1]
    rows = 2 * B
    loads = [
        pltpu.make_async_copy(route_hbm, route_ref, sems.at[0]),
        pltpu.make_async_copy(tok_hbm, tok_ref, sems.at[1]),
        pltpu.make_async_copy(sig_hbm, sig_ref, sems.at[2]),
    ]
    for load in loads:
        load.start()
    before = lax.broadcasted_iota(jnp.int32, (tokens, tokens), 0) < lax.broadcasted_iota(
        jnp.int32, (tokens, tokens), 1
    )
    before = ones_where(before)
    loads[0].wait()
    route = route_ref[...]
    hot = lax.broadcasted_iota(jnp.int32, (experts, tokens), 0) == route
    earlier = dot(ones_where(hot), before)
    position = jnp.sum(jnp.where(hot, earlier, 0.0), axis=0, keepdims=True)
    slot = route * SLOTS + position.astype(jnp.int32)
    line = lax.broadcasted_iota(jnp.int32, (rows, tokens), 0)
    stores = []
    for part, (source, col) in enumerate(((tok_ref, 0), (sig_ref, wide))):
        loads[1 + part].wait()
        for start in range(0, out_ref.shape[0], rows):
            at = (slice(start, start + rows), slice(col, col + source.shape[1]))
            pick = ones_where(line + start == slot)
            out_ref[at] = dot(pick, source[...]).astype(jnp.bfloat16)
            stores.append(pltpu.make_async_copy(out_ref.at[at], out_hbm.at[at], sems.at[3 + len(stores)]))
            stores[-1].start()
    for store in stores:
        store.wait()


def dispatch(route, tokens, signal, experts):
    count, wide = tokens.shape
    hidden = signal.shape[1]
    total = experts * SLOTS
    anywhere = pl.BlockSpec(memory_space=pl.ANY)
    return pl.pallas_call(
        functools.partial(dispatch_kernel, experts),
        in_specs=[anywhere] * 3,
        out_specs=anywhere,
        out_shape=jax.ShapeDtypeStruct((total, wide + hidden), jnp.bfloat16),
        scratch_shapes=[
            pltpu.VMEM((1, count), jnp.int32),
            pltpu.VMEM((count, wide), jnp.bfloat16),
            pltpu.VMEM((count, hidden), jnp.bfloat16),
            pltpu.VMEM((total, wide + hidden), jnp.bfloat16),
            pltpu.SemaphoreType.DMA((3 + 2 * (total // (2 * B)),)),
        ],
        compiler_params=params(60),
        cost_estimate=cost(2 * total * count * (wide + hidden), 6 * MIB),
        name="dispatch",
    )(route, tokens, signal)


def owned_blocks(d, group):
    found = [(d, d, 0, 0), (d, d, 0, 1), (d, d, 1, 1)]
    for h in range(group):
        if h > d:
            found += [(d, h, 0, 0), (d, h, 0, 1)]
        if h < d:
            found += [(h, d, 1, 0), (h, d, 1, 1)]
    return found


def gradient_kernel(group, scale, x_ref, grad_hbm, part_hbm, grad_ref, part_ref, sems):
    wide = grad_ref.shape[0]
    step = 2 * B
    lines = wide // step
    stores = []
    for r in range(lines):
        at = slice(r * step, (r + 1) * step)
        grad_ref[at, :] = (outer(x_ref[:, at], x_ref[:, wide:]) * scale).astype(jnp.bfloat16)
        stores.append(pltpu.make_async_copy(grad_ref.at[at, :], grad_hbm.at[at, :], sems.at[r]))
        stores[-1].start()
    place = {}
    for d in range(group):
        for k, name in enumerate(owned_blocks(d, group)):
            place[name] = (d, k)
    last = {d: max((p, q) for (p, q, _, _) in owned_blocks(d, group)) for d in range(group)}
    for p in range(group):
        for q in range(p, group):
            gram = outer(
                grad_ref[:, p * step : (p + 1) * step], grad_ref[:, q * step : (q + 1) * step]
            ).astype(jnp.bfloat16)
            for i in range(2):
                for j in range(2):
                    if (p, q, i, j) in place:
                        d, k = place[(p, q, i, j)]
                        part_ref[d, k * B : (k + 1) * B, :] = gram[
                            i * B : (i + 1) * B, j * B : (j + 1) * B
                        ]
            for d in range(group):
                if last[d] == (p, q):
                    stores.append(pltpu.make_async_copy(part_ref.at[d], part_hbm.at[d], sems.at[lines + d]))
                    stores[-1].start()
    for store in stores:
        store.wait()


def gradient(x, group, wide, scale):
    total, both = x.shape
    hidden = both - wide
    part = (group, PIECE * B, B)
    return pl.pallas_call(
        functools.partial(gradient_kernel, group, scale),
        in_specs=[vmem()],
        out_specs=(pl.BlockSpec(memory_space=pl.ANY),) * 2,
        out_shape=(
            jax.ShapeDtypeStruct((wide, hidden), jnp.bfloat16),
            jax.ShapeDtypeStruct(part, jnp.bfloat16),
        ),
        scratch_shapes=[
            pltpu.VMEM((wide, hidden), jnp.bfloat16),
            pltpu.VMEM(part, jnp.bfloat16),
            pltpu.SemaphoreType.DMA((wide // (2 * B) + group,)),
        ],
        compiler_params=params(16),
        cost_estimate=cost(2 * wide * hidden * (total + hidden), 10 * MIB),
        name="gradient",
    )(x)


def statistic_kernel(
    group, full, flags_ref, parts_ref, prev_ref, root_ref, stat_hbm, send_ref, stat_ref, own_ref, sem
):
    me, live = flags_ref[0], flags_ref[1]

    def gram(k):
        total = parts_ref[0, k * B : (k + 1) * B, :].astype(jnp.float32)
        for s in range(1, group):
            total += parts_ref[s, k * B : (k + 1) * B, :].astype(jnp.float32)
        return total

    def put(k, block, row, col):
        at = (slice(row, row + B), pl.ds(pl.multiple_of(col, B), B))
        new = KEEP * prev_ref[at] + (1.0 - KEEP) * block / full
        stat_ref[at] = new
        own_ref[k * B : (k + 1) * B, :] = new.astype(jnp.bfloat16)

    mine = pl.multiple_of(me * 2 * B, 2 * B)
    put(0, gram(0), 0, mine)
    put(1, gram(1), 0, mine + B)
    put(2, gram(2), B, mine + B)
    for j in range(group - 1):
        k = 3 + 2 * j

        @pl.when(j >= me)
        def _():
            col = (j + 1) * 2 * B
            put(k, gram(k), 0, col)
            put(k + 1, gram(k + 1), 0, col + B)

        @pl.when(j < me)
        def _():
            col = j * 2 * B + B
            put(k, gram(k).T, 0, col)
            put(k + 1, gram(k + 1).T, B, col)

    stat_ref[B:, pl.ds(mine, B)] = stat_ref[:B, pl.ds(mine + B, B)].T
    store = pltpu.make_async_copy(stat_ref, stat_hbm, sem)
    store.start()

    @pl.when(live != 0)
    def _():
        for t in range(group):
            send_ref[t] = own_ref[...]

    @pl.when(live == 0)
    def _():
        for t in range(group):
            for c in range(root_ref.shape[1] // B):
                at = slice(2 * B + c * REST, 2 * B + (c + 1) * REST)
                send_ref[t, at, :] = root_ref[-REST:, c * B : (c + 1) * B]
            send_ref[t, : 2 * B, :] = own_ref[pl.ds(shared(me, t), 2 * B), :]

    store.wait()


def shared(s, t):
    other = jnp.where(t > s, t - 1, jnp.minimum(t, PIECE // 2 - 2))
    return pl.multiple_of((3 + 2 * other) * B, B)


def new_statistic(flags, parts, prev, root, full):
    group = parts.shape[0]
    return pl.pallas_call(
        functools.partial(statistic_kernel, group, float(full)),
        in_specs=[smem(), vmem(), vmem(), vmem()],
        out_specs=(pl.BlockSpec(memory_space=pl.ANY), vmem()),
        out_shape=(
            jax.ShapeDtypeStruct(prev.shape, jnp.float32),
            jax.ShapeDtypeStruct((group, PIECE * B, B), jnp.bfloat16),
        ),
        scratch_shapes=[
            pltpu.VMEM(prev.shape, jnp.float32),
            pltpu.VMEM((PIECE * B, B), jnp.bfloat16),
            pltpu.SemaphoreType.DMA,
        ],
        compiler_params=params(8),
        cost_estimate=cost(4 * prev.size, 4 * MIB),
        name="statistic",
    )(flags, parts, prev, root)


def root_kernel(
    group,
    flags_ref,
    pieces_ref,
    prev_ref,
    up_1,
    up_2,
    up_3,
    down_1,
    down_2,
    down_3,
    grad_hbm,
    part_hbm,
    stat_hbm,
    rows_hbm,
    update_hbm,
    a_ref,
    f_ref,
    g_ref,
    h_ref,
    s_ref,
    grad_ref,
    mirror_ref,
    sems,
):
    me, live = flags_ref[0], flags_ref[1]
    order = a_ref.shape[0]
    step = 2 * B
    done = sems.at[2 * group - 2]
    load = pltpu.make_async_copy(grad_hbm, grad_ref, sems.at[2 * group - 1])
    rows_sem = sems.at[2 * group]
    load.start()

    def mirrored(j):
        s = jnp.where(j < me, j, j + 1)
        start = jnp.where(live != 0, shared(s, me), 0)
        col = pl.multiple_of(s * step, step)
        found = []
        for k in range(2):
            at = pl.ds(pl.multiple_of(start + k * B, B), B)
            mirror_ref[2 * j + k] = pieces_ref[s, at, :].astype(jnp.float32).T
            row = jnp.where(j < me, k * B, B)
            place = col + jnp.where(j < me, 0, k * B)
            target = stat_hbm.at[pl.ds(pl.multiple_of(row, B), B), pl.ds(pl.multiple_of(place, B), B)]
            found.append(pltpu.make_async_copy(mirror_ref.at[2 * j + k], target, sems.at[2 * j + k]))
        return found

    stores = []
    for j in range(group - 1):
        stores += mirrored(j)
        stores[-2].start()
        stores[-1].start()

    def rows_of(i, count=step):
        return pl.ds(pl.multiple_of(i * step, step), count)

    @pl.when(live == 0)
    def _():
        pltpu.make_async_copy(prev_ref, rows_hbm, rows_sem).start()
        for s in range(group):
            for c in range(order // B):
                at = slice(2 * B + c * REST, 2 * B + (c + 1) * REST)
                g_ref[(s + 1) * step - REST : (s + 1) * step, c * B : (c + 1) * B] = pieces_ref[s, at, :]
        g_ref[rows_of(me, step - REST), :] = prev_ref[: step - REST, :]
        for k, (below, above) in enumerate(((up_1, down_1), (up_2, down_2), (up_3, down_3)), 1):

            @pl.when(me >= k)
            def _():
                g_ref[rows_of(me - k, step - REST), :] = below[...]

            @pl.when(me + k < group)
            def _():
                g_ref[rows_of(me + k, step - REST), :] = above[...]

    @pl.when(live != 0)
    def _():
        def fill(block, row, col, mirror=True):
            a_ref[row : row + B, col : col + B] = block
            if mirror:
                a_ref[col : col + B, row : row + B] = block.T

        for s in range(group):
            at = s * step
            block = [pieces_ref[s, k * B : (k + 1) * B, :] for k in range(PIECE)]
            fill(block[0], at, at, False)
            fill(block[1], at, at + B)
            fill(block[2], at + B, at + B, False)
            k = 3
            for h in range(group):
                if h > s:
                    fill(block[k], at, h * step)
                    fill(block[k + 1], at, h * step + B)
                if h < s:
                    fill(block[k], at, h * step + B)
                    fill(block[k + 1], at + B, h * step + B)
                if h != s:
                    k += 2

        lines = range(order // step)
        row = lax.broadcasted_iota(jnp.int32, (step, step), 0)
        eye = row == lax.broadcasted_iota(jnp.int32, (step, step), 1)

        def both(ref, i, j, block):
            ref[i * step : (i + 1) * step, j * step : (j + 1) * step] = block
            if i != j:
                ref[j * step : (j + 1) * step, i * step : (i + 1) * step] = block.T

        def piece(ref, i, j):
            return ref[i * step : (i + 1) * step, j * step : (j + 1) * step]

        def upper_product(left, right, use):
            for i in lines:
                found = dot(left[i * step : (i + 1) * step, :], right[:, i * step :])
                for j in lines[i:]:
                    use(i, j, found[:, (j - i) * step : (j - i + 1) * step])

        largest = jnp.zeros((1, step), jnp.float32)
        for i in lines:
            diagonal = jnp.where(eye, piece(a_ref, i, i).astype(jnp.float32), 0.0)
            largest = jnp.maximum(largest, jnp.max(diagonal, axis=0, keepdims=True))
        unit = 1.0 / jnp.max(largest, axis=1, keepdims=True)

        def squared(i, j, block):
            s_ref[i * step : (i + 1) * step, j * step : (j + 1) * step] = block
            both(g_ref, i, j, (block * unit * unit).astype(jnp.bfloat16))

        upper_product(a_ref, a_ref, squared)

        def applied(vector, matrix_ref):
            image = dot(vector.astype(jnp.bfloat16), matrix_ref[...])
            length = jnp.sqrt(jnp.sum(image * image, axis=1, keepdims=True))
            return image / length, length

        vector = jnp.full((16, order), 1.0 / math.sqrt(order), jnp.float32)
        vector = lax.fori_loop(0, POWER // 2 - 1, lambda _, v: applied(v, g_ref)[0], vector)
        vector, _ = applied(vector, a_ref)
        _, length = applied(vector, a_ref)
        scaling = 2.5 / length[:1, :1]
        quarter = jnp.sqrt(jnp.sqrt(scaling)) * 0.25

        for i in lines:
            for j in lines[i:]:
                moment = scaling * piece(a_ref, i, j).astype(jnp.float32)
                twice = scaling * (scaling * piece(s_ref, i, j))
                square = twice - 10.0 * moment
                if i == j:
                    square += jnp.where(eye, 25.0, 0.0)
                both(g_ref, i, j, (square * 0.0625).astype(jnp.bfloat16))
                both(h_ref, i, j, ((5.0 * moment - twice) * 0.25).astype(jnp.bfloat16))

        upper_product(g_ref, g_ref, lambda i, j, block: both(f_ref, i, j, block.astype(jnp.bfloat16)))

        def root(i, j, tail):
            factor = -1.25 * scaling * piece(a_ref, i, j).astype(jnp.float32)
            if i == j:
                factor += jnp.where(eye, 6.25, 0.0)
            both(g_ref, i, j, ((factor - tail) * quarter).astype(jnp.bfloat16))

        upper_product(f_ref, h_ref, root)
        pltpu.make_async_copy(g_ref.at[rows_of(me), :], rows_hbm, rows_sem).start()

    load.wait()

    def line(i, _):
        here = rows_of(i)
        f_ref[here, :] = dot(grad_ref[here, :], g_ref[...]).astype(jnp.bfloat16)
        pltpu.make_async_copy(f_ref.at[here, :], update_hbm.at[here, :], done).start()
        return 0

    lax.fori_loop(0, order // step, line, 0)
    pltpu.make_async_copy(f_ref, update_hbm, done).wait()
    pltpu.make_async_copy(prev_ref, rows_hbm, rows_sem).wait()

    for store in stores:
        store.wait()


def inverse_root(flags, pieces, prev, uppers, grad, part):
    group = pieces.shape[0]
    _, order = grad.shape
    square = pltpu.VMEM((order, order), jnp.bfloat16)
    anywhere = pl.BlockSpec(memory_space=pl.ANY)
    return pl.pallas_call(
        functools.partial(root_kernel, group),
        in_specs=[smem()] + [vmem()] * (2 * group) + [anywhere] * 2,
        out_specs=(anywhere, anywhere, anywhere),
        out_shape=(
            jax.ShapeDtypeStruct(part.shape, jnp.float32),
            jax.ShapeDtypeStruct(prev.shape, jnp.bfloat16),
            jax.ShapeDtypeStruct(grad.shape, jnp.bfloat16),
        ),
        input_output_aliases={10: 0, 9: 2},
        scratch_shapes=[square] * 4
        + [
            pltpu.VMEM((order, order), jnp.float32),
            pltpu.VMEM(grad.shape, jnp.bfloat16),
            pltpu.VMEM((2 * (group - 1), B, B), jnp.float32),
            pltpu.SemaphoreType.DMA((2 * group + 1,)),
        ],
        compiler_params=params(26),
        cost_estimate=cost(10 * order**3, 8 * MIB),
        name="root",
    )(flags, pieces, prev, *uppers, grad, part)


def step_of(tokens, cotangent, routing, stat_prev, root_prev, owner_map):
    experts = lax.axis_size("expert")
    group = lax.axis_size("group")
    my_expert = lax.axis_index("expert")
    me = lax.axis_index("group").astype(jnp.int32)
    rows, wide = tokens.shape
    order = cotangent.shape[1]
    owners = experts // 4
    live = (jnp.take(owner_map, my_expert) < owners).astype(jnp.int32)
    flags = jnp.stack([me, live])

    def passed(x, way):
        pairs = [(g, g + way) for g in range(group) if 0 <= g + way < group]
        return lax.ppermute(x, "group", pairs)

    prev = root_prev[0]
    upper = prev[: prev.shape[0] - REST]
    ups = [passed(upper, 1)]
    downs = [passed(upper, -1)]
    sent = dispatch(routing.reshape(1, rows), tokens, cotangent, experts)
    sent = sent.reshape(experts, SLOTS, wide + order)
    got = lax.all_to_all(sent, "expert", 0, 0, tiled=True)
    for _ in range(2, group):
        ups.append(passed(ups[-1], 1))
        downs.append(passed(downs[-1], -1))
    got, *uppers = lax.optimization_barrier((got, *ups, *downs))
    grad, part = gradient(got.reshape(experts * SLOTS, -1), group, wide, 1.0 / math.sqrt(rows))
    parts = lax.all_to_all(part, "group", 0, 0, tiled=True)
    stat_own, send = new_statistic(flags, parts, stat_prev[0], prev, wide * group)
    pieces = lax.all_to_all(send, "group", 0, 0, tiled=True)
    stat, root_rows, update = inverse_root(flags, pieces, prev, uppers, grad, stat_own)
    return stat[None], root_rows[None], update[None]


def solution(mesh):
    in_specs = (
        P("expert", "group"),
        P("expert", None),
        P("expert", None),
        P("expert", "group", None),
        P("expert", "group", None),
        P(),
    )
    out_specs = (P("expert", "group", None), P("expert", "group", None), P("expert", "group", None))
    return jax.shard_map(step_of, mesh=mesh, in_specs=in_specs, out_specs=out_specs, check_vma=False)
```
